32 devices in a mesh: rows: 32 (over z, y, x, core).
Axes of the slice: x: 2, y: 2, z: 4, core: 2. Of those that a mesh axis runs over, the one named last changes fastest.
Arguments:
- coupling: float32 [128, 5, 128, 128], P('rows'), may hold values from -0.15 to 3.15, as said below
- columns: int32 [128, 5], replicated, may hold values from 0 to 63, as said below
- row_slots: int32 [64], replicated, may hold values from 0 to 127, as said below
Outputs:
- inverse_estimate: float32 [128, 5, 128, 128], P('rows')
The draws below stay inside these ranges and needn't reach their ends.
Inputs may be any that keep to these rules, and one draw needn't show every extreme that they name: `coupling`: in every slot the diagonal entries of tile 0 are at least 0.3. `columns`: for a slot that holds block row r, entry 0 is r and the other 4 entries are distinct block rows (r + d) mod 64 with 1 <= |d| <= 3; entries of slots that hold no block row mean nothing. `row_slots`: device i owns slots i * 4 to (i + 1) * 4 - 1. Block rows are owned in order: device 0 holds the first ones, each device a contiguous run of rows in its first slots, at least 1 and at most 4 rows; some device holds 4.
All inputs are finite; a program needn't handle non-finite values.
Results may differ from the reference program's by a relative error of at most 0.0003.
Values sent between devices are 32-bit elements; how exact they have to be, the bound alone decides.
No kernel may reach another device: no remote copies, remote signals or barrier semaphores. Data moves between devices by JAX's collectives and lax.ppermute only.
A program may use at most 64 MiB of HBM per device.

```python
import math
import jax
import jax.numpy as jnp
import numpy as np
from jax import lax

TILE = 128
ROW_TILES = 5
BAND = 3
ROWS_DEV = 2
SLOT_DEV = 4
BLOCK_ROWS = 64
SLOTS = 128


def layout(key):
    devices = BLOCK_ROWS // ROWS_DEV
    quads = devices // 4
    key_kind, key_order, key_pick, key_fill = jax.random.split(jax.random.fold_in(key, 7), 4)
    table = jnp.array(np.array([[4, 2, 1, 1], [3, 3, 1, 1], [2, 2, 2, 2], [3, 2, 2, 1]], np.int32))
    kinds = jax.random.randint(key_kind, (quads,), 0, 4).at[0].set(0)
    units = jnp.take(table, kinds, axis=0)
    scores = jax.random.randint(key_order, (quads, 4), 0, 1024) * 4 + jnp.arange(4, dtype=jnp.int32)
    units = jnp.take_along_axis(units, jnp.argsort(scores, axis=1), axis=1)
    counts = units.reshape(-1) * (ROWS_DEV // 2)
    starts = jnp.cumsum(counts) - counts
    every_row = jnp.arange(BLOCK_ROWS, dtype=jnp.int32)
    owners = jnp.sum((starts[None, :] <= every_row[:, None]).astype(jnp.int32), axis=1) - 1
    row_slots = owners * SLOT_DEV + every_row - jnp.take(starts, owners)
    reach = jnp.concatenate([jnp.arange(-BAND, 0), jnp.arange(1, BAND + 1)]).astype(jnp.int32)
    picks = jax.random.randint(key_pick, (BLOCK_ROWS, 2 * BAND), 0, 1 << 20) * (2 * BAND) + jnp.arange(2 * BAND, dtype=jnp.int32)
    chosen = jnp.argsort(picks, axis=1)[:, :ROW_TILES - 1]
    neighbours = (every_row[:, None] + jnp.take(reach, chosen)) % BLOCK_ROWS
    row_columns = jnp.concatenate([every_row[:, None], neighbours], axis=1)
    filler = jax.random.randint(key_fill, (SLOTS, ROW_TILES), 0, BLOCK_ROWS)
    columns = filler.at[row_slots].set(row_columns)
    return (columns, row_slots)


def draw_columns(key, part):
    return layout(key)[0]


def draw_row_slots(key, part):
    return layout(key)[1]


def draw_coupling(key, part):
    key_off, key_diag = jax.random.split(jax.random.fold_in(key, 3))
    shape = (SLOTS, ROW_TILES, TILE, TILE)
    deviation = 0.11 / math.sqrt(TILE)
    spread = jnp.clip(jax.random.normal(key_off, shape, jnp.float32), -6.0, 6.0) * deviation
    scales = jnp.exp(jax.random.uniform(key_diag, (SLOTS, TILE), jnp.float32, math.log(0.5), math.log(2.0)))
    identity = jnp.eye(TILE, dtype=jnp.float32)
    leading = (jnp.arange(ROW_TILES) == 0).astype(jnp.float32)
    return spread + leading[None, :, None, None] * scales[:, None, :, None] * identity


def setup_inputs(seed: int = 0) -> dict:
    arg_keys = jax.random.split(jax.random.key(seed), 4)
    return {
        "coupling": draw_coupling(jax.random.fold_in(arg_keys[3], 71), 0),
        "columns": draw_columns(jax.random.fold_in(arg_keys[3], 71), 0),
        "row_slots": draw_row_slots(jax.random.fold_in(arg_keys[3], 71), 0),
    }


precise = lax.Precision.HIGHEST


def locate(wanted, row_ids):
    matches = wanted[..., None] == row_ids
    return jnp.argmax(matches, axis=-1).astype(jnp.int32)


def start_iterate(coupling, inverse, column_inverse):
    identity = jnp.eye(coupling.shape[-1], dtype=coupling.dtype)
    leading = (jnp.arange(coupling.shape[1]) == 0).astype(coupling.dtype)
    diagonal_part = 2.0 * leading[None, :, None, None] * (inverse[:, None, :, None] * identity)
    return diagonal_part - inverse[:, None, :, None] * coupling * column_inverse[:, :, None, :]


def pattern_product(left, row_pool, row_ids, pool_columns, own_columns):
    def per_slot(operands):
        blocks, row_columns = operands
        located = locate(row_columns, row_ids)
        fetched = jnp.take(row_pool, located, axis=0)
        their_columns = jnp.take(pool_columns, located, axis=0)
        selector = (their_columns[:, :, None] == row_columns[None, None, :]).astype(row_pool.dtype)
        chosen = jnp.einsum("kab,kaqr->kbqr", selector, fetched, precision=precise)
        return jnp.einsum("kpq,kbqr->bpr", blocks, chosen, precision=precise)

    return lax.map(per_slot, (left, own_columns))


def reference(coupling, columns, row_slots):
    blocks = jnp.take(coupling, row_slots, axis=0)
    row_columns = jnp.take(columns, row_slots, axis=0)
    inverse = 1.0 / jnp.diagonal(blocks[:, 0], axis1=1, axis2=2)
    column_inverse = jnp.take(inverse, row_columns, axis=0)
    first_iterate = start_iterate(blocks, inverse, column_inverse)
    every_row = jnp.arange(BLOCK_ROWS, dtype=jnp.int32)
    product = pattern_product(blocks, first_iterate, every_row, row_columns, row_columns)
    second_iterate = 2.0 * first_iterate - pattern_product(first_iterate, product, every_row, row_columns, row_columns)
    return jnp.zeros_like(coupling).at[row_slots].set(second_iterate)
```

```python
import jax
import jax.numpy as jnp
from jax import lax
from jax.experimental import pallas as pl
from jax.experimental.pallas import tpu as pltpu
from jax.sharding import PartitionSpec as P

BAND = 3
REACH = 2 * BAND
GROUP = 2
SHIFTS = 3


def distance_tiles(row_tiles):
    return {d: row_tiles if d <= BAND else REACH - d + 1 for d in range(1, REACH + 1)}


def message_plan(row_tiles):
    tiles = distance_tiles(row_tiles)
    plan = []
    base = 0
    for shift in range(1, SHIFTS + 1):
        first = GROUP * (shift - 1) + 1
        places = {}
        size = 0
        for d in range(first, REACH + 1):
            places[d] = size
            size += tiles[d]
        plan.append((places, size, base))
        base += size
    return plan, base


def group_starts(row_slots, slot_count, devices, own_index):
    groups = devices // GROUP
    group = own_index // GROUP
    steps = jnp.arange(-SHIFTS, SHIFTS + 2, dtype=jnp.int32)
    wanted = group + steps
    turns = jnp.floor_divide(wanted, groups)
    firsts = jnp.concatenate([(wanted - turns * groups) * GROUP, group[None] * GROUP + 1])
    turns = jnp.concatenate([turns, jnp.zeros((1,), jnp.int32)])
    below = (row_slots[None, :] < (firsts * slot_count)[:, None]).astype(jnp.int32)
    starts = jnp.sum(below, axis=1) + turns * row_slots.shape[0]
    return jnp.concatenate([starts, (own_index % GROUP)[None]])


class Rows:
    def __init__(self, starts, row_slots, columns, core, row_tiles, slot_count):
        self.starts = starts
        self.row_slots = row_slots
        self.columns = columns
        self.core = core
        self.row_tiles = row_tiles
        self.slot_count = slot_count
        self.rows = row_slots.shape[0]
        self.plan, self.message = message_plan(row_tiles)

    def group(self, step):
        return self.starts[SHIFTS + step]

    @property
    def middle(self):
        return self.starts[2 * SHIFTS + 2]

    def wrapped(self, row):
        row = jnp.where(row < 0, row + self.rows, row)
        return jnp.where(row >= self.rows, row - self.rows, row)

    def offset(self, row, t):
        row = self.wrapped(row)
        d = self.columns[self.row_slots[row] * self.row_tiles + t] - row
        d = jnp.where(d > self.rows // 2, d - self.rows, d)
        return jnp.where(d < -(self.rows // 2), d + self.rows, d)

    def group_tile(self, row):
        low = self.group(0)
        middle = self.middle
        slot = jnp.where(row < middle, row - low, row - middle + self.slot_count)
        return jnp.clip(slot, 0, GROUP * self.slot_count - 1) * self.row_tiles

    def tile_at(self, row, offset):
        found = jnp.int32(0)
        for t in range(1, self.row_tiles):
            found = jnp.where(self.offset(row, t) == offset, t, found)
        return found

    def source(self, row):
        low = self.group(0)
        high = self.group(1)
        behind = row < low
        ahead = row >= high
        distance = jnp.where(behind, low - row, row - high + 1)
        near = jnp.where(behind, low - self.group(-1), self.group(2) - high)
        middle = jnp.where(behind, low - self.group(-2), self.group(3) - high)
        place = jnp.int32(0)
        for shift in reversed(range(SHIFTS)):
            places, _, base = self.plan[shift]
            found = jnp.int32(0)
            for d, at in places.items():
                found = jnp.where(distance == d, base + at, found)
            if shift == SHIFTS - 1:
                place = found
            else:
                place = jnp.where(distance <= (near, middle)[shift], found, place)
        held = GROUP * self.slot_count * self.row_tiles
        beyond = held + jnp.where(behind, 0, self.message) + place
        outside = behind | ahead
        return jnp.where(outside, beyond, self.group_tile(row)), jnp.where(outside, distance, 0)


def split(value):
    high = value.astype(jnp.bfloat16)
    return high, (value - high.astype(jnp.float32)).astype(jnp.bfloat16)


def eye(tile):
    return lax.broadcasted_iota(jnp.int32, (tile, tile), 0) == lax.broadcasted_iota(
        jnp.int32, (tile, tile), 1
    )


def inverse_column(block):
    tile = block.shape[-1]
    return 1.0 / jnp.sum(jnp.where(eye(tile), block, 0.0), axis=1, keepdims=True)


def inverse_row(block):
    tile = block.shape[-1]
    return 1.0 / jnp.sum(jnp.where(eye(tile), block, 0.0), axis=0, keepdims=True)


def pack_kernel(row_tiles, slot_count, starts, row_slots, columns, own, other, *rest):
    outs = rest[:SHIFTS]
    pool, sems = rest[SHIFTS:]
    core = starts[2 * SHIFTS + 3]
    rows = Rows(starts, row_slots, columns, core, row_tiles, slot_count)
    held = slot_count * row_tiles
    own_copy = pltpu.make_async_copy(own, pool.at[pl.ds(core * held, held)], sems.at[0])
    other_copy = pltpu.make_async_copy(other, pool.at[pl.ds((1 - core) * held, held)], sems.at[1])
    own_copy.start()
    other_copy.start()
    own_copy.wait()
    other_copy.wait()
    forward = core == 1
    sign = jnp.where(forward, 1, -1)
    for shift in range(1, SHIFTS + 1):
        places, _, _ = rows.plan[shift - 1]
        edge = jnp.where(forward, rows.group(shift), rows.group(1 - shift))
        for d, at in places.items():
            row = jnp.where(forward, edge - d, edge + d - 1)
            base = rows.group_tile(row)
            row = jnp.clip(row, rows.group(0), rows.group(1) - 1)
            if d <= BAND:
                for t in range(row_tiles):
                    outs[shift - 1][at + t] = pool[base + t]
            else:
                scale = -inverse_column(pool[base])
                for step in range(d - BAND, BAND + 1):
                    t = rows.tile_at(row, sign * step)
                    outs[shift - 1][at + step - (d - BAND)] = scale * pool[base + t]


def compute_kernel(row_tiles, slot_count, starts, row_slots, columns, own, other, *rest):
    received = rest[:SHIFTS]
    passed = rest[SHIFTS : 2 * SHIFTS]
    out = rest[2 * SHIFTS]
    (pool, left_high, left_low, y_high, y_low, p_high, p_low, g_high, g_low, z_high, z_low,
     inv_row, offsets, y_at, p_at, sems) = rest[2 * SHIFTS + 1 :]
    core = starts[2 * SHIFTS + 3]
    rows = Rows(starts, row_slots, columns, core, row_tiles, slot_count)
    held = slot_count * row_tiles
    tile = own.shape[-1]
    width = 2 * BAND + 1
    copies = [
        pltpu.make_async_copy(own, pool.at[pl.ds(core * held, held)], sems.at[0]),
        pltpu.make_async_copy(other, pool.at[pl.ds((1 - core) * held, held)], sems.at[1]),
    ]
    for shift in range(SHIFTS):
        _, size, base = rows.plan[shift]
        mine = GROUP * held + (1 - core) * rows.message + base
        theirs = GROUP * held + core * rows.message + base
        copies.append(
            pltpu.make_async_copy(
                received[shift], pool.at[pl.ds(mine, size)], sems.at[2 + 2 * shift]
            )
        )
        copies.append(
            pltpu.make_async_copy(
                passed[shift], pool.at[pl.ds(theirs, size)], sems.at[3 + 2 * shift]
            )
        )
    for copy in copies:
        copy.start()

    first = jnp.where(core == 0, rows.group(0), rows.middle)
    count = jnp.where(core == 0, rows.middle, rows.group(1)) - first
    near = count + 2 * BAND
    zero_y = y_high.shape[0] - 1
    zero_p = p_high.shape[0] - 1
    nothing = jnp.zeros((tile, tile), jnp.bfloat16)
    y_high[zero_y] = nothing
    y_low[zero_y] = nothing
    p_high[zero_p] = nothing
    p_low[zero_p] = nothing

    def clear_y(i, _):
        y_at[i] = zero_y
        return _

    def clear_p(i, _):
        p_at[i] = zero_p
        return _

    lax.fori_loop(0, y_at.shape[0], clear_y, 0)
    lax.fori_loop(0, p_at.shape[0], clear_p, 0)
    for copy in copies:
        copy.wait()

    def invert(f, _):
        base, _d = rows.source(first - BAND + f)
        inv_row[f] = inverse_row(pool[base])
        return _

    lax.fori_loop(0, near, invert, 0)

    def near_row(f, _):
        row = first - BAND + f
        base, _d = rows.source(row)
        column = inverse_column(pool[base])
        for t in range(row_tiles):
            offset = rows.offset(row, t)
            offsets[f * row_tiles + t] = offset
            block = pool[base + t]
            high, low = split(block)
            left_high[f, :, pl.ds(t * tile, tile)] = high
            left_low[f, :, pl.ds(t * tile, tile)] = low
            c = f + offset
            inside = (c >= 0) & (c < near)
            value = -(column * block) * inv_row[jnp.clip(c, 0, near - 1)]
            if t == 0:
                value = value + jnp.where(eye(tile), 2.0 * column, 0.0)
            high, low = split(value)
            at = (f + BAND) * width + offset + BAND
            y_high[at] = high
            y_low[at] = low
            y_at[at] = jnp.where(inside, at, zero_y)
            p_at[f * width + offset + BAND] = f * row_tiles + t
        return _

    lax.fori_loop(0, near, near_row, 0)

    def far_row(e, _):
        behind = e < BAND
        sign = jnp.where(behind, 1, -1)
        d = jnp.where(behind, REACH - e, e + 1)
        w = jnp.where(behind, e, near + e)
        row = first - REACH + w
        base, beyond = rows.source(row)
        whole = beyond <= BAND
        scale = jnp.where(whole, -inverse_column(pool[base]), 1.0)
        for step in range(1, BAND + 1):
            offset = sign * step
            t = rows.tile_at(row, offset)
            present = (t > 0) & (step >= d - BAND)
            skip = jnp.clip(step - (beyond - BAND), 0, BAND)
            at = w * width + offset + BAND

            @pl.when(present)
            def keep():
                block = pool[base + jnp.where(whole, t, skip)]
                c = jnp.clip(w - BAND + offset, 0, near - 1)
                high, low = split((scale * block) * inv_row[c])
                y_high[at] = high
                y_low[at] = low
                y_at[at] = at

        return _

    lax.fori_loop(0, 2 * BAND, far_row, 0)

    def gather(table, limit, zero, high_ref, low_ref, f):
        for t in range(row_tiles):
            step = offsets[f * row_tiles + t]
            for v in range(row_tiles):
                ahead = offsets[f * row_tiles + v] - step
                inside = (ahead >= -BAND) & (ahead <= BAND)
                at = (limit + step) * width + jnp.clip(ahead, -BAND, BAND) + BAND
                at = jnp.where(inside, table[at], zero)
                g_high[pl.ds(t * tile, tile), pl.ds(v * tile, tile)] = high_ref[at]
                g_low[pl.ds(t * tile, tile), pl.ds(v * tile, tile)] = low_ref[at]

    def dot(a, b):
        return jnp.dot(a, b, preferred_element_type=jnp.float32)

    def product_row(f, _):
        gather(y_at, f + BAND, zero_y, y_high, y_low, f)
        a_high = left_high[f]
        value = dot(a_high, g_high[...]) + dot(a_high, g_low[...]) + dot(left_low[f], g_high[...])
        for t in range(row_tiles):
            high, low = split(value[:, t * tile : (t + 1) * tile])
            p_high[f * row_tiles + t] = high
            p_low[f * row_tiles + t] = low
        return _

    lax.fori_loop(0, near, product_row, 0)

    def own_row(j, _):
        f = j + BAND
        gather(p_at, f, zero_p, p_high, p_low, f)
        for t in range(row_tiles):
            at = (f + BAND) * width + offsets[f * row_tiles + t] + BAND
            z_high[:, pl.ds(t * tile, tile)] = y_high[at]
            z_low[:, pl.ds(t * tile, tile)] = y_low[at]
        high = z_high[...]
        low = z_low[...]
        value = dot(high, g_high[...]) + dot(high, g_low[...]) + dot(low, g_high[...])
        value = 2.0 * (high.astype(jnp.float32) + low.astype(jnp.float32)) - value
        for t in range(row_tiles):
            out[j * row_tiles + t] = value[:, t * tile : (t + 1) * tile]
        return _

    lax.fori_loop(0, count, own_row, 0)

    def empty_row(j, _):
        for t in range(row_tiles):
            out[j * row_tiles + t] = jnp.zeros((tile, tile), jnp.float32)
        return _

    lax.fori_loop(count, slot_count, empty_row, 0)


def shards(coupling, columns, row_slots):
    slot_count, row_tiles, tile, _ = coupling.shape
    devices = lax.axis_size("rows")
    own_index = lax.axis_index("rows")
    plan, message = message_plan(row_tiles)
    held = slot_count * row_tiles
    near = slot_count + 2 * BAND
    width = 2 * BAND + 1
    own = coupling.reshape(held, tile, tile)
    listed = range(devices)
    partner = [(i, i ^ 1) for i in listed]
    other = lax.ppermute(own, "rows", partner)
    starts = group_starts(row_slots, slot_count, devices, own_index)
    flat_columns = columns.reshape(-1)
    smem = pl.BlockSpec(memory_space=pltpu.SMEM)
    hbm = pl.BlockSpec(memory_space=pltpu.HBM)
    vmem = pl.BlockSpec(memory_space=pltpu.VMEM)
    messages = pl.pallas_call(
        lambda *refs: pack_kernel(row_tiles, slot_count, *refs),
        out_shape=[jax.ShapeDtypeStruct((size, tile, tile), jnp.float32) for _, size, _ in plan],
        in_specs=[smem] * 3 + [hbm] * 2,
        out_specs=[vmem] * SHIFTS,
        scratch_shapes=[
            pltpu.VMEM((GROUP * held, tile, tile), jnp.float32),
            pltpu.SemaphoreType.DMA((2,)),
        ],
        name="pack",
    )(starts, row_slots, flat_columns, own, other)
    received = []
    for shift in range(1, SHIFTS + 1):
        step = GROUP * shift
        pairs = [(i, (i + step if i % GROUP else i - step) % devices) for i in listed]
        received.append(lax.ppermute(messages[shift - 1], "rows", pairs))
    passed = [lax.ppermute(value, "rows", partner) for value in received]
    out = pl.pallas_call(
        lambda *refs: compute_kernel(row_tiles, slot_count, *refs),
        out_shape=jax.ShapeDtypeStruct((held, tile, tile), jnp.float32),
        in_specs=[smem] * 3 + [hbm] * (2 + 2 * SHIFTS),
        out_specs=vmem,
        scratch_shapes=[
            pltpu.VMEM((GROUP * held + 2 * message, tile, tile), jnp.float32),
            pltpu.VMEM((near, tile, row_tiles * tile), jnp.bfloat16),
            pltpu.VMEM((near, tile, row_tiles * tile), jnp.bfloat16),
            pltpu.VMEM(((near + 2 * BAND) * width + 1, tile, tile), jnp.bfloat16),
            pltpu.VMEM(((near + 2 * BAND) * width + 1, tile, tile), jnp.bfloat16),
            pltpu.VMEM((near * row_tiles + 1, tile, tile), jnp.bfloat16),
            pltpu.VMEM((near * row_tiles + 1, tile, tile), jnp.bfloat16),
            pltpu.VMEM((row_tiles * tile, row_tiles * tile), jnp.bfloat16),
            pltpu.VMEM((row_tiles * tile, row_tiles * tile), jnp.bfloat16),
            pltpu.VMEM((tile, row_tiles * tile), jnp.bfloat16),
            pltpu.VMEM((tile, row_tiles * tile), jnp.bfloat16),
            pltpu.VMEM((near, 1, tile), jnp.float32),
            pltpu.SMEM((near * row_tiles,), jnp.int32),
            pltpu.SMEM(((near + 2 * BAND) * width,), jnp.int32),
            pltpu.SMEM((near * width,), jnp.int32),
            pltpu.SemaphoreType.DMA((2 + 2 * SHIFTS,)),
        ],
        name="compute",
    )(starts, row_slots, flat_columns, own, other, *received, *passed)
    return out.reshape(coupling.shape)


def solution(mesh):
    return jax.shard_map(
        shards,
        mesh=mesh,
        in_specs=(P("rows", None, None, None), P(), P()),
        out_specs=P("rows", None, None, None),
        check_vma=False,
    )
```

```python
import jax
import jax.numpy as jnp
from jax import lax
from jax.experimental import pallas as pl
from jax.experimental.pallas import tpu as pltpu
from jax.sharding import PartitionSpec as P


BAND = 3
REACH = 2 * BAND
GROUP = 2
SHIFTS = 3
STARTS = 2 * SHIFTS + 4

FAR = [(d, step) for d in range(BAND + 1, REACH + 1) for step in range(d - BAND, BAND + 1)]


def far_slots(shift):
    return [(d, step) for d, step in FAR if d > GROUP * (shift - 1)]


def group_starts(row_slots, slot_count, devices, own_index):
    groups = devices // GROUP
    group = own_index // GROUP
    steps = jnp.arange(-SHIFTS, SHIFTS + 2, dtype=jnp.int32)
    wanted = group + steps
    turns = jnp.floor_divide(wanted, groups)
    firsts = jnp.concatenate([(wanted - turns * groups) * GROUP, group[None] * GROUP + 1])
    turns = jnp.concatenate([turns, jnp.zeros((1,), jnp.int32)])
    below = (row_slots[None, :] < (firsts * slot_count)[:, None]).astype(jnp.int32)
    starts = jnp.sum(below, axis=1) + turns * row_slots.shape[0]
    return jnp.concatenate([starts, (own_index % GROUP)[None]])


def pattern_table(starts, row_slots, columns, slot_count):
    rows = row_slots.shape[0]
    span = GROUP * slot_count + 2 * REACH
    row = starts[SHIFTS] - REACH + jnp.arange(span, dtype=jnp.int32)
    row = jnp.where(row < 0, row + rows, row)
    row = jnp.where(row >= rows, row - rows, row)
    found = jnp.take(columns, jnp.take(row_slots, row), axis=0) - row[:, None]
    found = jnp.where(found > rows // 2, found - rows, found)
    found = jnp.where(found < -(rows // 2), found + rows, found)
    wanted = jnp.arange(-BAND, BAND + 1, dtype=jnp.int32)
    order = jnp.arange(1, columns.shape[1] + 1, dtype=jnp.int32)
    which = jnp.sum(jnp.where(found[:, None, :] == wanted[None, :, None], order, 0), axis=2) - 1
    return jnp.concatenate([starts, jnp.clip(found, -BAND, BAND).reshape(-1), which.reshape(-1)])


class Rows:
    def __init__(self, table, row_tiles, slot_count):
        self.table = table
        self.row_tiles = row_tiles
        self.slot_count = slot_count
        self.core = table[STARTS - 1]
        self.middle = table[STARTS - 2]
        self.offsets = STARTS
        self.which = STARTS + (GROUP * slot_count + 2 * REACH) * row_tiles

    def group(self, step):
        return self.table[SHIFTS + step]

    def edge(self, shift, forward):
        return jnp.where(forward, self.group(shift), self.group(1 - shift))

    def place(self, row):
        return jnp.clip(row - self.group(0) + REACH, 0, GROUP * self.slot_count + 2 * REACH - 1)

    def offset(self, row, t):
        return self.table[self.offsets + self.place(row) * self.row_tiles + t]

    def tile_at(self, row, offset):
        return self.table[self.which + self.place(row) * (2 * BAND + 1) + offset + BAND]

    def group_tile(self, row):
        low = self.group(0)
        middle = self.middle
        slot = jnp.where(row < middle, row - low, row - middle + self.slot_count)
        return jnp.clip(slot, 0, GROUP * self.slot_count - 1) * self.row_tiles


def split(value):
    high = value.astype(jnp.bfloat16)
    return high, (value - high.astype(jnp.float32)).astype(jnp.bfloat16)


def eye(tile):
    return lax.broadcasted_iota(jnp.int32, (tile, tile), 0) == lax.broadcasted_iota(
        jnp.int32, (tile, tile), 1
    )


def inverse_column(block):
    tile = block.shape[-1]
    return 1.0 / jnp.sum(jnp.where(eye(tile), block, 0.0), axis=1, keepdims=True)


def inverse_row(block):
    tile = block.shape[-1]
    return 1.0 / jnp.sum(jnp.where(eye(tile), block, 0.0), axis=0, keepdims=True)


def near_pack_kernel(row_tiles, slot_count, starts, own, other, near, next_near, sems):
    rows = Rows(starts, row_tiles, slot_count)
    forward = rows.core == 0
    held = slot_count * row_tiles
    wanted = []
    for shift, ref, distances in ((1, near, range(2, BAND + 1)), (2, next_near, (BAND,))):
        for i, d in enumerate(distances):
            edge = rows.edge(shift, forward)
            base = rows.group_tile(jnp.where(forward, edge - d, edge + d - 1))
            wanted.append((base, ref.at[pl.ds(i * row_tiles, row_tiles)]))
    for i, (base, place) in enumerate(wanted):
        second = base >= held
        mine = jnp.where(second, 1, 0) == rows.core
        start = jnp.where(second, base - held, base)

        @pl.when(mine)
        def take_own():
            pltpu.make_async_copy(own.at[pl.ds(start, row_tiles)], place, sems.at[i]).start()

        @pl.when(jnp.logical_not(mine))
        def take_other():
            pltpu.make_async_copy(other.at[pl.ds(start, row_tiles)], place, sems.at[i]).start()

    for i, (base, place) in enumerate(wanted):
        pltpu.make_async_copy(own.at[pl.ds(0, row_tiles)], place, sems.at[i]).wait()


def far_pack_kernel(row_tiles, slot_count, starts, own, other, *rest):
    outs = rest[:SHIFTS]
    pool, sems = rest[SHIFTS:]
    core = starts[STARTS - 1]
    rows = Rows(starts, row_tiles, slot_count)
    held = slot_count * row_tiles
    own_copy = pltpu.make_async_copy(own, pool.at[pl.ds(core * held, held)], sems.at[0])
    other_copy = pltpu.make_async_copy(other, pool.at[pl.ds((1 - core) * held, held)], sems.at[1])
    own_copy.start()
    other_copy.start()
    own_copy.wait()
    other_copy.wait()
    forward = core == 0
    sign = jnp.where(forward, 1, -1)
    for shift in range(1, SHIFTS + 1):
        edge = rows.edge(shift, forward)
        slots = far_slots(shift)
        for d in sorted({d for d, _ in slots}):
            row = jnp.where(forward, edge - d, edge + d - 1)
            base = rows.group_tile(row)
            scale = -inverse_column(pool[base])
            for at, (distance, step) in enumerate(slots):
                if distance == d:
                    t = rows.tile_at(row, sign * step)
                    factor = jnp.where(t > 0, scale, 0.0)
                    outs[shift - 1][at] = factor * pool[base + jnp.maximum(t, 0)]


def dot(a, b):
    return jnp.dot(a, b, preferred_element_type=jnp.float32)


def near_kernel(row_tiles, slot_count, starts, own, other, edge, near_rows, next_rows,
                edge_p, near_p, next_p, out, a_high, a_low, b_high, b_low, inv_out,
                pool, left_high, left_low, y_high, y_low, p_high, p_low,
                inv_row, offsets, y_at, p_at, whole, sems):
    core = starts[2 * SHIFTS + 3]
    rows = Rows(starts, row_tiles, slot_count)
    tile = own.shape[-1]
    width = 2 * BAND + 1
    first = jnp.where(core == 0, rows.group(0), rows.middle)
    count = jnp.where(core == 0, rows.middle, rows.group(1)) - first
    near = count + 2 * BAND
    low = rows.group(0)
    high = rows.group(1)
    near_behind = low - rows.group(-1)
    near_ahead = rows.group(2) - high
    zero_y = y_high.shape[0] - 1
    zero_p = p_high.shape[0] - 1
    nothing = jnp.zeros((tile, tile), jnp.bfloat16)
    y_high[zero_y] = nothing
    y_low[zero_y] = nothing
    p_high[zero_p] = nothing
    p_low[zero_p] = nothing

    def fetch(w, carry):
        row = first - REACH + w
        behind = row < low
        ahead = row >= high
        outside = behind | ahead
        inside = jnp.logical_not(outside)
        d = jnp.where(behind, low - row, row - high + 1)
        reached = jnp.where(behind, near_behind, near_ahead)
        mine = outside & (jnp.where(behind, 0, 1) == core)
        theirs = outside & (jnp.where(behind, 0, 1) != core)
        home = inside & (jnp.where(row < rows.middle, 0, 1) == core)
        slot = jnp.where(row < rows.middle, row - low, row - rows.middle)
        whole[w] = jnp.where(inside | (d <= BAND), 1, 0)
        choices = [(home, own, slot), (inside & jnp.logical_not(home), other, slot)]
        for side, refs in ((mine, (edge, near_rows, next_rows)), (theirs, (edge_p, near_p, next_p))):
            choices.append((side & (d == 1), refs[0], 0))
            choices.append((side & (d > 1) & (d <= BAND) & (d <= reached), refs[1], d - 2))
            choices.append((side & (d == BAND) & (d > reached), refs[2], 0))
        for chosen, ref, at in choices:

            @pl.when(chosen)
            def take():
                pltpu.make_async_copy(
                    ref.at[pl.ds(at * row_tiles, row_tiles)], pool.at[pl.ds(w * row_tiles, row_tiles)], sems.at[w]
                ).start()

        return carry

    lax.fori_loop(0, near + 2 * BAND, fetch, 0)

    def clear_y(i, carry):
        y_at[i] = zero_y
        return carry

    def clear_p(i, carry):
        p_at[i] = zero_p
        return carry

    lax.fori_loop(0, y_at.shape[0], clear_y, 0, unroll=8)
    lax.fori_loop(0, p_at.shape[0], clear_p, 0, unroll=7)

    def arrive(w, carry):
        @pl.when(whole[w] == 1)
        def wait():
            place = pool.at[pl.ds(w * row_tiles, row_tiles)]
            pltpu.make_async_copy(own.at[pl.ds(0, row_tiles)], place, sems.at[w]).wait()

        return carry

    lax.fori_loop(0, near + 2 * BAND, arrive, 0)

    def invert(f, carry):
        inv_row[f] = inverse_row(pool[(f + BAND) * row_tiles])
        return carry

    lax.fori_loop(0, near, invert, 0)

    def near_row(f, carry):
        row = first - BAND + f
        base = (f + BAND) * row_tiles
        column = inverse_column(pool[base])
        for t in range(row_tiles):
            offset = rows.offset(row, t)
            offsets[f * row_tiles + t] = offset
            block = pool[base + t]
            high_part, low_part = split(block)
            left_high[f, :, pl.ds(t * tile, tile)] = high_part
            left_low[f, :, pl.ds(t * tile, tile)] = low_part
            c = f + offset
            inside = (c >= 0) & (c < near)
            value = -(column * block) * inv_row[jnp.clip(c, 0, near - 1)]
            if t == 0:
                value = value + jnp.where(eye(tile), 2.0 * column, 0.0)
            high_part, low_part = split(value)
            at = (f + BAND) * width + offset + BAND
            y_high[at] = high_part
            y_low[at] = low_part
            y_at[at] = jnp.where(inside, at, zero_y)
            p_at[f * width + offset + BAND] = f * row_tiles + t
        return carry

    lax.fori_loop(0, near, near_row, 0)

    def far_row(e, carry):
        behind = e < BAND
        sign = jnp.where(behind, 1, -1)
        d = jnp.where(behind, REACH - e, e + 1)
        w = jnp.where(behind, e, near + e)
        row = first - REACH + w

        @pl.when(whole[w] == 1)
        def build():
            scale = -inverse_column(pool[w * row_tiles])
            for step in range(1, BAND + 1):
                offset = sign * step
                t = rows.tile_at(row, offset)
                at = w * width + offset + BAND

                @pl.when((t > 0) & (step >= d - BAND))
                def keep():
                    c = jnp.clip(w - BAND + offset, 0, near - 1)
                    high_part, low_part = split((scale * pool[w * row_tiles + t]) * inv_row[c])
                    y_high[at] = high_part
                    y_low[at] = low_part
                    y_at[at] = at

        return carry

    lax.fori_loop(0, 2 * BAND, far_row, 0)

    def gathered(table, start, zero, high_ref, low_ref, f, lefts):
        steps = [offsets[f * row_tiles + t] for t in range(row_tiles)]
        at = []
        for t in range(row_tiles):
            line = []
            for v in range(row_tiles):
                ahead = steps[v] - steps[t]
                inside = (ahead >= -BAND) & (ahead <= BAND)
                place = (start + steps[t]) * width + jnp.clip(ahead, -BAND, BAND) + BAND
                line.append(jnp.where(inside, table[place], zero))
            at.append(line)
        left_h, left_l = lefts
        results = []
        for v in range(0, row_tiles, 2):
            pair = range(v, min(v + 2, row_tiles))

            def right(ref):
                lines = [jnp.concatenate([ref[at[t][c]] for c in pair], axis=1) for t in range(row_tiles)]
                return jnp.concatenate(lines, axis=0)

            high_right = right(high_ref)
            value = dot(left_h, high_right) + dot(left_l, high_right) + dot(left_h, right(low_ref))
            for i in range(len(pair)):
                results.append(value[:, i * tile : (i + 1) * tile])
        return results

    def product_row(f, carry):
        values = gathered(y_at, f + BAND, zero_y, y_high, y_low, f, (left_high[f], left_low[f]))
        for t, value in enumerate(values):
            high_part, low_part = split(value)
            p_high[f * row_tiles + t] = high_part
            p_low[f * row_tiles + t] = low_part
        return carry

    lax.fori_loop(0, near, product_row, 0)

    def own_row(j, carry):
        f = j + BAND
        tiles = []
        for t in range(row_tiles):
            at = (f + BAND) * width + offsets[f * row_tiles + t] + BAND
            tiles.append((y_high[at], y_low[at]))
        lefts = [jnp.concatenate([pair[i] for pair in tiles], axis=1) for i in range(2)]
        values = gathered(p_at, f, zero_p, p_high, p_low, f, lefts)
        for t, value in enumerate(values):
            high_part, low_part = tiles[t]
            out[j * row_tiles + t] = 2.0 * (high_part.astype(jnp.float32) + low_part.astype(jnp.float32)) - value
        return carry

    lax.fori_loop(0, count, own_row, 0)

    def empty_row(j, carry):
        for t in range(row_tiles):
            out[j * row_tiles + t] = jnp.zeros((tile, tile), jnp.float32)
        return carry

    lax.fori_loop(count, slot_count, empty_row, 0)

    a_high[...] = jnp.zeros_like(a_high)
    a_low[...] = jnp.zeros_like(a_low)
    b_high[...] = jnp.zeros_like(b_high)
    b_low[...] = jnp.zeros_like(b_low)
    for side in range(2):
        sign = -1 if side == 0 else 1
        for e in range(1, BAND + 1):
            f = BAND - e if side == 0 else near - BAND + e - 1
            row = first - BAND + f
            inv_out[side * BAND + e - 1] = inv_row[f]
            for d in range(BAND + 1, REACH + 1):
                if d - e <= BAND:
                    t = rows.tile_at(row, sign * (d - e))
                    here = (side, pl.ds((e - 1) * tile, tile), pl.ds((d - BAND - 1) * tile, tile))

                    @pl.when(t > 0)
                    def keep_a():
                        lanes = pl.ds(pl.multiple_of(t * tile, tile), tile)
                        a_high[here] = left_high[f, :, lanes]
                        a_low[here] = left_low[f, :, lanes]

            for i in range(BAND + 1 - e):
                w = REACH + i if side == 0 else REACH + count - 1 - i
                at = y_at[w * width + sign * (i + e) + BAND]
                here = (side, pl.ds(i * tile, tile), pl.ds((e - 1) * tile, tile))

                @pl.when(i < count)
                def keep_b():
                    b_high[here] = y_high[at]
                    b_low[here] = y_low[at]


def far_kernel(row_tiles, slot_count, starts, estimate, a_high_in, a_low_in, b_high_in, b_low_in, inv_in, *rest):
    arrays = rest[: 2 * SHIFTS]
    out, a_high, a_low, b_high, b_low, inv_rows, far, changed, y_high, y_low, sems, row_sems = rest[2 * SHIFTS :]
    core = starts[STARTS - 1]
    rows = Rows(starts, row_tiles, slot_count)
    tile = changed.shape[-1]
    first = jnp.where(core == 0, rows.group(0), rows.middle)
    count = jnp.where(core == 0, rows.middle, rows.group(1)) - first
    pairs = [(a_high_in, a_high), (a_low_in, a_low), (b_high_in, b_high), (b_low_in, b_low), (inv_in, inv_rows)]
    base = 0
    bases = []
    for array in arrays:
        bases.append(base)
        pairs.append((array, far.at[pl.ds(base, array.shape[0])]))
        base += array.shape[0]
    copies = [pltpu.make_async_copy(*pair, sems.at[i]) for i, pair in enumerate(pairs)]
    for copy in reversed(copies):
        copy.start()
    targets = []
    for side in range(2):
        sign = -1 if side == 0 else 1
        for i in range(BAND):
            for e in range(1, BAND + 1 - i):
                j = i if side == 0 else count - 1 - i
                t = rows.tile_at(first + j, sign * (i + e))
                targets.append((side, i, e, (i < count) & (t > 0), j * row_tiles + t))
    for at, (side, i, e, present, place) in enumerate(targets):

        @pl.when(present)
        def read():
            pltpu.make_async_copy(estimate.at[place], changed.at[at], row_sems.at[at]).start()

    y_high[...] = jnp.zeros_like(y_high)
    y_low[...] = jnp.zeros_like(y_low)
    for copy in copies[4:]:
        copy.wait()
    for side in range(2):
        direct = core == side
        between = jnp.where(direct, 0, first - rows.group(0) if side == 0 else rows.group(1) - first - count)
        one = rows.group(0) - rows.group(-1) if side == 0 else rows.group(2) - rows.group(1)
        two = rows.group(0) - rows.group(-2) if side == 0 else rows.group(3) - rows.group(1)
        for d, step in FAR:
            e = d - step
            here = (side, pl.ds((d - BAND - 1) * tile, tile), pl.ds((e - 1) * tile, tile))
            beyond = d - between
            place = jnp.int32(0)
            for distance, other_step in FAR:
                if other_step == step and distance <= d:
                    for shift in reversed(range(1, SHIFTS + 1)):
                        slots = far_slots(shift)
                        if (distance, step) in slots:
                            at = slots.index((distance, step))
                            at = jnp.where(direct, bases[shift - 1] + at, bases[SHIFTS + shift - 1] + at)
                            held = jnp.bool_(True) if shift == SHIFTS else beyond <= (one, two)[shift - 1]
                            place = jnp.where((beyond == distance) & held, at, place)
            value = jnp.where(beyond > BAND, far[place] * inv_rows[side * BAND + e - 1], 0.0)
            high_part, low_part = split(value)
            y_high[here] = high_part
            y_low[here] = low_part
    for copy in copies[:4]:
        copy.wait()
    for side in range(2):
        sign = -1 if side == 0 else 1
        extra = dot(a_high[side], y_high[side]) + dot(a_high[side], y_low[side])
        extra = extra + dot(a_low[side], y_high[side])
        bands = []
        for k in range(1, BAND + 1):
            parts = []
            for e in range(1, BAND + 1):
                part = extra[(k - 1) * tile : k * tile, (e - 1) * tile : e * tile]
                if k != e:
                    row = first - k if side == 0 else first + count + k - 1
                    part = jnp.where(rows.tile_at(row, sign * (e - k)) > 0, part, 0.0)
                parts.append(part)
            bands.append(jnp.concatenate(parts, axis=1))
        extra_high, extra_low = split(jnp.concatenate(bands, axis=0))
        change = dot(b_high[side], extra_high) + dot(b_high[side], extra_low)
        change = change + dot(b_low[side], extra_high)
        for at, (of, i, e, present, place) in enumerate(targets):
            if of == side:
                part = change[i * tile : (i + 1) * tile, (e - 1) * tile : e * tile]

                @pl.when(present)
                def update():
                    pltpu.make_async_copy(estimate.at[place], changed.at[at], row_sems.at[at]).wait()
                    changed[at] -= part
                    pltpu.make_async_copy(changed.at[at], out.at[place], row_sems.at[at]).start()

    for at, (side, i, e, present, place) in enumerate(targets):

        @pl.when(present)
        def finish():
            pltpu.make_async_copy(changed.at[at], out.at[place], row_sems.at[at]).wait()


def estimate_rows(coupling, columns, row_slots):
    slot_count, row_tiles, tile, _ = coupling.shape
    devices = lax.axis_size("rows")
    own_index = lax.axis_index("rows")
    held = slot_count * row_tiles
    near = slot_count + 2 * BAND
    width = 2 * BAND + 1
    reach = BAND * tile
    own = coupling.reshape(held, tile, tile)
    listed = range(devices)
    smem = pl.BlockSpec(memory_space=pltpu.SMEM)
    hbm = pl.BlockSpec(memory_space=pltpu.HBM)
    vmem = pl.BlockSpec(memory_space=pltpu.VMEM)

    def blocks(count, dtype=jnp.float32):
        return jax.ShapeDtypeStruct((count, tile, tile), dtype)

    def partner(value):
        return lax.ppermute(value, "rows", [(i, i ^ 1) for i in listed])

    def along(value, step):
        return lax.ppermute(value, "rows", [(i, (i + (-step if i % GROUP else step)) % devices) for i in listed])

    other = partner(own)
    starts = group_starts(row_slots, slot_count, devices, own_index)
    last = starts[SHIFTS + 1] - 1 - starts[2 * SHIFTS + 2]
    edge_row = jnp.where(own_index % GROUP == 0, 0, last) * row_tiles
    edge_out = lax.dynamic_slice_in_dim(own, edge_row, row_tiles, 0)
    edge = along(edge_out, -1)
    near_out, next_out = pl.pallas_call(
        lambda *refs: near_pack_kernel(row_tiles, slot_count, *refs),
        out_shape=[blocks((BAND - 1) * row_tiles), blocks(row_tiles)],
        in_specs=[smem] + [hbm] * 2,
        out_specs=[vmem] * 2,
        scratch_shapes=[pltpu.SemaphoreType.DMA((BAND,))],
        name="near_pack",
    )(starts, own, other)
    near_rows = along(near_out, GROUP)
    next_rows = along(next_out, 2 * GROUP)
    table = pattern_table(lax.optimization_barrier((starts, near_out))[0], row_slots, columns, slot_count)
    far_out = pl.pallas_call(
        lambda *refs: far_pack_kernel(row_tiles, slot_count, *refs),
        out_shape=[blocks(len(far_slots(shift))) for shift in range(1, SHIFTS + 1)],
        in_specs=[smem] + [hbm] * 2,
        out_specs=[vmem] * SHIFTS,
        scratch_shapes=[
            pltpu.VMEM((GROUP * held, tile, tile), jnp.float32),
            pltpu.SemaphoreType.DMA((2,)),
        ],
        name="far_pack",
    )(table, own, other)
    passed = []
    for value in (edge, near_rows, next_rows):
        passed.append(partner(value))
    far_out = lax.optimization_barrier((tuple(far_out), near_rows))[0]
    far_in = []
    for shift in range(1, SHIFTS + 1):
        far_in.append(along(far_out[shift - 1], GROUP * shift))
    rows_of = near * row_tiles
    table_size = (near + 2 * BAND) * width
    side_block = jax.ShapeDtypeStruct((2, reach, reach), jnp.bfloat16)
    estimate, *shares = pl.pallas_call(
        lambda *refs: near_kernel(row_tiles, slot_count, *refs),
        out_shape=[blocks(held)] + [side_block] * 4 + [jax.ShapeDtypeStruct((2 * BAND, 1, tile), jnp.float32)],
        in_specs=[smem] + [hbm] * 8,
        out_specs=[vmem] * 6,
        scratch_shapes=[
            pltpu.VMEM(((near + 2 * BAND) * row_tiles, tile, tile), jnp.float32),
            pltpu.VMEM((near, tile, row_tiles * tile), jnp.bfloat16),
            pltpu.VMEM((near, tile, row_tiles * tile), jnp.bfloat16),
            pltpu.VMEM((table_size + 1, tile, tile), jnp.bfloat16),
            pltpu.VMEM((table_size + 1, tile, tile), jnp.bfloat16),
            pltpu.VMEM((rows_of + 1, tile, tile), jnp.bfloat16),
            pltpu.VMEM((rows_of + 1, tile, tile), jnp.bfloat16),
            pltpu.VMEM((near, 1, tile), jnp.float32),
            pltpu.SMEM((rows_of,), jnp.int32),
            pltpu.SMEM((table_size,), jnp.int32),
            pltpu.SMEM((near * width,), jnp.int32),
            pltpu.SMEM((near + 2 * BAND,), jnp.int32),
            pltpu.SemaphoreType.DMA((near + 2 * BAND,)),
        ],
        cost_estimate=pl.CostEstimate(flops=4 * 10**9, bytes_accessed=10**7, transcendentals=0),
        name="near_rows",
    )(table, own, other, edge, near_rows, next_rows, *passed)
    far_passed = []
    for shift in range(1, SHIFTS + 1):
        far_passed.append(partner(far_in[shift - 1]))
    targets = BAND * (BAND + 1)
    out = pl.pallas_call(
        lambda *refs: far_kernel(row_tiles, slot_count, *refs),
        out_shape=blocks(held),
        in_specs=[smem] + [hbm] * (6 + 2 * SHIFTS),
        out_specs=hbm,
        scratch_shapes=[pltpu.VMEM((2, reach, reach), jnp.bfloat16)] * 4
        + [
            pltpu.VMEM((2 * BAND, 1, tile), jnp.float32),
            pltpu.VMEM((2 * sum(len(far_slots(shift)) for shift in range(1, SHIFTS + 1)), tile, tile), jnp.float32),
            pltpu.VMEM((targets, tile, tile), jnp.float32),
            pltpu.VMEM((2, reach, reach), jnp.bfloat16),
            pltpu.VMEM((2, reach, reach), jnp.bfloat16),
            pltpu.SemaphoreType.DMA((5 + 2 * SHIFTS,)),
            pltpu.SemaphoreType.DMA((targets,)),
        ],
        input_output_aliases={1: 0},
        name="far_rows",
    )(table, estimate, *shares, *far_in, *far_passed)
    return out.reshape(coupling.shape)


def solution(mesh):
    return jax.shard_map(
        estimate_rows,
        mesh=mesh,
        in_specs=(P("rows", None, None, None), P(), P()),
        out_specs=P("rows", None, None, None),
        check_vma=False,
    )
```

```python
import jax
import jax.numpy as jnp
from jax import lax
from jax.experimental import pallas as pl
from jax.experimental.pallas import tpu as pltpu
from jax.sharding import PartitionSpec as P


BAND = 3
REACH = 2 * BAND
GROUP = 2
SHIFTS = 3
STARTS = 2 * SHIFTS + 4

FAR = [(d, step) for d in range(BAND + 1, REACH + 1) for step in range(d - BAND, BAND + 1)]


def far_slots(shift):
    return [(d, step) for d, step in FAR if d > GROUP * (shift - 1)]


def group_starts(row_slots, slot_count, devices, own_index):
    groups = devices // GROUP
    group = own_index // GROUP
    steps = jnp.arange(-SHIFTS, SHIFTS + 2, dtype=jnp.int32)
    wanted = group + steps
    turns = jnp.floor_divide(wanted, groups)
    firsts = jnp.concatenate([(wanted - turns * groups) * GROUP, group[None] * GROUP + 1])
    turns = jnp.concatenate([turns, jnp.zeros((1,), jnp.int32)])
    below = (row_slots[None, :] < (firsts * slot_count)[:, None]).astype(jnp.int32)
    starts = jnp.sum(below, axis=1) + turns * row_slots.shape[0]
    return jnp.concatenate([starts, (own_index % GROUP)[None]])


def pattern_table(starts, row_slots, columns, slot_count):
    rows = row_slots.shape[0]
    span = GROUP * slot_count + 2 * REACH
    row = starts[SHIFTS] - REACH + jnp.arange(span, dtype=jnp.int32)
    row = jnp.where(row < 0, row + rows, row)
    row = jnp.where(row >= rows, row - rows, row)
    found = jnp.take(columns, jnp.take(row_slots, row), axis=0) - row[:, None]
    found = jnp.where(found > rows // 2, found - rows, found)
    found = jnp.where(found < -(rows // 2), found + rows, found)
    wanted = jnp.arange(-BAND, BAND + 1, dtype=jnp.int32)
    order = jnp.arange(1, columns.shape[1] + 1, dtype=jnp.int32)
    which = jnp.sum(jnp.where(found[:, None, :] == wanted[None, :, None], order, 0), axis=2) - 1
    return jnp.concatenate([starts, jnp.clip(found, -BAND, BAND).reshape(-1), which.reshape(-1)])


class Rows:
    def __init__(self, table, row_tiles, slot_count):
        self.table = table
        self.row_tiles = row_tiles
        self.slot_count = slot_count
        self.core = table[STARTS - 1]
        self.middle = table[STARTS - 2]
        self.offsets = STARTS
        self.which = STARTS + (GROUP * slot_count + 2 * REACH) * row_tiles

    def group(self, step):
        return self.table[SHIFTS + step]

    def edge(self, shift, forward):
        return jnp.where(forward, self.group(shift), self.group(1 - shift))

    def place(self, row):
        return jnp.clip(row - self.group(0) + REACH, 0, GROUP * self.slot_count + 2 * REACH - 1)

    def offset(self, row, t):
        return self.table[self.offsets + self.place(row) * self.row_tiles + t]

    def tile_at(self, row, offset):
        return self.table[self.which + self.place(row) * (2 * BAND + 1) + offset + BAND]

    def group_tile(self, row):
        low = self.group(0)
        middle = self.middle
        slot = jnp.where(row < middle, row - low, row - middle + self.slot_count)
        return jnp.clip(slot, 0, GROUP * self.slot_count - 1) * self.row_tiles


def split(value):
    high = value.astype(jnp.bfloat16)
    return high, (value - high.astype(jnp.float32)).astype(jnp.bfloat16)


def eye(tile):
    return lax.broadcasted_iota(jnp.int32, (tile, tile), 0) == lax.broadcasted_iota(
        jnp.int32, (tile, tile), 1
    )


def inverse_column(block):
    tile = block.shape[-1]
    return 1.0 / jnp.sum(jnp.where(eye(tile), block, 0.0), axis=1, keepdims=True)


def inverse_row(block):
    tile = block.shape[-1]
    return 1.0 / jnp.sum(jnp.where(eye(tile), block, 0.0), axis=0, keepdims=True)


def near_pack_kernel(row_tiles, slot_count, starts, own, other, near, next_near, sems):
    rows = Rows(starts, row_tiles, slot_count)
    forward = rows.core == 0
    held = slot_count * row_tiles
    wanted = []
    for shift, ref, distances in ((1, near, range(2, BAND + 1)), (2, next_near, (BAND,))):
        for i, d in enumerate(distances):
            edge = rows.edge(shift, forward)
            base = rows.group_tile(jnp.where(forward, edge - d, edge + d - 1))
            wanted.append((base, ref.at[pl.ds(i * row_tiles, row_tiles)]))
    for i, (base, place) in enumerate(wanted):
        second = base >= held
        mine = jnp.where(second, 1, 0) == rows.core
        start = jnp.where(second, base - held, base)

        @pl.when(mine)
        def take_own():
            pltpu.make_async_copy(own.at[pl.ds(start, row_tiles)], place, sems.at[i]).start()

        @pl.when(jnp.logical_not(mine))
        def take_other():
            pltpu.make_async_copy(other.at[pl.ds(start, row_tiles)], place, sems.at[i]).start()

    for i, (base, place) in enumerate(wanted):
        pltpu.make_async_copy(own.at[pl.ds(0, row_tiles)], place, sems.at[i]).wait()


def far_pack_kernel(row_tiles, slot_count, starts, own, other, *rest):
    outs = rest[:SHIFTS]
    pool, sems = rest[SHIFTS:]
    core = starts[STARTS - 1]
    rows = Rows(starts, row_tiles, slot_count)
    held = slot_count * row_tiles
    own_copy = pltpu.make_async_copy(own, pool.at[pl.ds(core * held, held)], sems.at[0])
    other_copy = pltpu.make_async_copy(other, pool.at[pl.ds((1 - core) * held, held)], sems.at[1])
    own_copy.start()
    other_copy.start()
    own_copy.wait()
    other_copy.wait()
    forward = core == 0
    sign = jnp.where(forward, 1, -1)
    for shift in range(1, SHIFTS + 1):
        edge = rows.edge(shift, forward)
        slots = far_slots(shift)
        for d in sorted({d for d, _ in slots}):
            row = jnp.where(forward, edge - d, edge + d - 1)
            base = rows.group_tile(row)
            scale = -inverse_column(pool[base])
            for at, (distance, step) in enumerate(slots):
                if distance == d:
                    t = rows.tile_at(row, sign * step)
                    factor = jnp.where(t > 0, scale, 0.0)
                    outs[shift - 1][at] = factor * pool[base + jnp.maximum(t, 0)]


def dot(a, b):
    return jnp.dot(a, b, preferred_element_type=jnp.float32)


def near_kernel(row_tiles, slot_count, starts, own, other, edge, near_rows, next_rows,
                edge_p, near_p, next_p, out, a_high, a_low, b_high, b_low, inv_out,
                pool, left_high, left_low, y_high, y_low, p_high, p_low,
                inv_row, offsets, y_at, p_at, whole, sems):
    core = starts[2 * SHIFTS + 3]
    rows = Rows(starts, row_tiles, slot_count)
    tile = own.shape[-1]
    width = 2 * BAND + 1
    first = jnp.where(core == 0, rows.group(0), rows.middle)
    count = jnp.where(core == 0, rows.middle, rows.group(1)) - first
    near = count + 2 * BAND
    low = rows.group(0)
    high = rows.group(1)
    near_behind = low - rows.group(-1)
    near_ahead = rows.group(2) - high
    zero_y = y_high.shape[0] - 1
    zero_p = p_high.shape[0] - 1
    nothing = jnp.zeros((tile, tile), jnp.bfloat16)
    y_high[zero_y] = nothing
    y_low[zero_y] = nothing
    p_high[zero_p] = nothing
    p_low[zero_p] = nothing

    def fetch(w, carry):
        row = first - REACH + w
        behind = row < low
        ahead = row >= high
        outside = behind | ahead
        inside = jnp.logical_not(outside)
        d = jnp.where(behind, low - row, row - high + 1)
        reached = jnp.where(behind, near_behind, near_ahead)
        mine = outside & (jnp.where(behind, 0, 1) == core)
        theirs = outside & (jnp.where(behind, 0, 1) != core)
        home = inside & (jnp.where(row < rows.middle, 0, 1) == core)
        slot = jnp.where(row < rows.middle, row - low, row - rows.middle)
        whole[w] = jnp.where(inside | (d <= BAND), 1, 0)
        choices = [(home, own, slot), (inside & jnp.logical_not(home), other, slot)]
        for side, refs in ((mine, (edge, near_rows, next_rows)), (theirs, (edge_p, near_p, next_p))):
            choices.append((side & (d == 1), refs[0], 0))
            choices.append((side & (d > 1) & (d <= BAND) & (d <= reached), refs[1], d - 2))
            choices.append((side & (d == BAND) & (d > reached), refs[2], 0))
        for chosen, ref, at in choices:

            @pl.when(chosen)
            def take():
                pltpu.make_async_copy(
                    ref.at[pl.ds(at * row_tiles, row_tiles)], pool.at[pl.ds(w * row_tiles, row_tiles)], sems.at[w]
                ).start()

        return carry

    lax.fori_loop(0, near + 2 * BAND, fetch, 0)

    def clear_y(i, carry):
        y_at[i] = zero_y
        return carry

    def clear_p(i, carry):
        p_at[i] = zero_p
        return carry

    lax.fori_loop(0, y_at.shape[0], clear_y, 0, unroll=8)
    lax.fori_loop(0, p_at.shape[0], clear_p, 0, unroll=7)

    def arrive(w, carry):
        @pl.when(whole[w] == 1)
        def wait():
            place = pool.at[pl.ds(w * row_tiles, row_tiles)]
            pltpu.make_async_copy(own.at[pl.ds(0, row_tiles)], place, sems.at[w]).wait()

        return carry

    lax.fori_loop(0, near + 2 * BAND, arrive, 0)

    def invert(f, carry):
        inv_row[f] = inverse_row(pool[(f + BAND) * row_tiles])
        return carry

    lax.fori_loop(0, near, invert, 0)

    def near_row(f, carry):
        row = first - BAND + f
        base = (f + BAND) * row_tiles
        column = inverse_column(pool[base])
        for t in range(row_tiles):
            offset = rows.offset(row, t)
            offsets[f * row_tiles + t] = offset
            block = pool[base + t]
            high_part, low_part = split(block)
            left_high[f, :, pl.ds(t * tile, tile)] = high_part
            left_low[f, :, pl.ds(t * tile, tile)] = low_part
            c = f + offset
            inside = (c >= 0) & (c < near)
            value = -(column * block) * inv_row[jnp.clip(c, 0, near - 1)]
            if t == 0:
                value = value + jnp.where(eye(tile), 2.0 * column, 0.0)
            high_part, low_part = split(value)
            at = (f + BAND) * width + offset + BAND
            y_high[at] = high_part
            y_low[at] = low_part
            y_at[at] = jnp.where(inside, at, zero_y)
            p_at[f * width + offset + BAND] = f * row_tiles + t
        return carry

    lax.fori_loop(0, near, near_row, 0)

    def far_row(e, carry):
        behind = e < BAND
        sign = jnp.where(behind, 1, -1)
        d = jnp.where(behind, REACH - e, e + 1)
        w = jnp.where(behind, e, near + e)
        row = first - REACH + w

        @pl.when(whole[w] == 1)
        def build():
            scale = -inverse_column(pool[w * row_tiles])
            for step in range(1, BAND + 1):
                offset = sign * step
                t = rows.tile_at(row, offset)
                at = w * width + offset + BAND

                @pl.when((t > 0) & (step >= d - BAND))
                def keep():
                    c = jnp.clip(w - BAND + offset, 0, near - 1)
                    high_part, low_part = split((scale * pool[w * row_tiles + t]) * inv_row[c])
                    y_high[at] = high_part
                    y_low[at] = low_part
                    y_at[at] = at

        return carry

    lax.fori_loop(0, 2 * BAND, far_row, 0)

    def gathered(table, start, zero, high_ref, low_ref, f, lefts):
        steps = [offsets[f * row_tiles + t] for t in range(row_tiles)]
        at = []
        for t in range(row_tiles):
            line = []
            for v in range(row_tiles):
                ahead = steps[v] - steps[t]
                inside = (ahead >= -BAND) & (ahead <= BAND)
                place = (start + steps[t]) * width + jnp.clip(ahead, -BAND, BAND) + BAND
                line.append(jnp.where(inside, table[place], zero))
            at.append(line)
        left_h, left_l = lefts
        results = []
        for v in range(0, row_tiles, 2):
            pair = range(v, min(v + 2, row_tiles))

            def right(ref):
                lines = [jnp.concatenate([ref[at[t][c]] for c in pair], axis=1) for t in range(row_tiles)]
                return jnp.concatenate(lines, axis=0)

            high_right = right(high_ref)
            value = dot(left_h, high_right) + dot(left_l, high_right) + dot(left_h, right(low_ref))
            for i in range(len(pair)):
                results.append(value[:, i * tile : (i + 1) * tile])
        return results

    def product_row(f, carry):
        values = gathered(y_at, f + BAND, zero_y, y_high, y_low, f, (left_high[f], left_low[f]))
        for t, value in enumerate(values):
            high_part, low_part = split(value)
            p_high[f * row_tiles + t] = high_part
            p_low[f * row_tiles + t] = low_part
        return carry

    lax.fori_loop(0, near, product_row, 0)

    def own_row(j, carry):
        f = j + BAND
        tiles = []
        for t in range(row_tiles):
            at = (f + BAND) * width + offsets[f * row_tiles + t] + BAND
            tiles.append((y_high[at], y_low[at]))
        lefts = [jnp.concatenate([pair[i] for pair in tiles], axis=1) for i in range(2)]
        values = gathered(p_at, f, zero_p, p_high, p_low, f, lefts)
        for t, value in enumerate(values):
            high_part, low_part = tiles[t]
            out[j * row_tiles + t] = 2.0 * (high_part.astype(jnp.float32) + low_part.astype(jnp.float32)) - value
        return carry

    lax.fori_loop(0, count, own_row, 0)

    def empty_row(j, carry):
        for t in range(row_tiles):
            out[j * row_tiles + t] = jnp.zeros((tile, tile), jnp.float32)
        return carry

    lax.fori_loop(count, slot_count, empty_row, 0)

    a_high[...] = jnp.zeros_like(a_high)
    a_low[...] = jnp.zeros_like(a_low)
    b_high[...] = jnp.zeros_like(b_high)
    b_low[...] = jnp.zeros_like(b_low)
    for side in range(2):
        sign = -1 if side == 0 else 1
        for e in range(1, BAND + 1):
            f = BAND - e if side == 0 else near - BAND + e - 1
            row = first - BAND + f
            inv_out[side * BAND + e - 1] = inv_row[f]
            for d in range(BAND + 1, REACH + 1):
                if d - e <= BAND:
                    t = rows.tile_at(row, sign * (d - e))
                    here = (side, pl.ds((e - 1) * tile, tile), pl.ds((d - BAND - 1) * tile, tile))

                    @pl.when(t > 0)
                    def keep_a():
                        lanes = pl.ds(pl.multiple_of(t * tile, tile), tile)
                        a_high[here] = left_high[f, :, lanes]
                        a_low[here] = left_low[f, :, lanes]

            for i in range(BAND + 1 - e):
                w = REACH + i if side == 0 else REACH + count - 1 - i
                at = y_at[w * width + sign * (i + e) + BAND]
                here = (side, pl.ds(i * tile, tile), pl.ds((e - 1) * tile, tile))

                @pl.when(i < count)
                def keep_b():
                    b_high[here] = y_high[at]
                    b_low[here] = y_low[at]


def far_kernel(row_tiles, slot_count, starts, estimate, a_high_in, a_low_in, b_high_in, b_low_in, inv_in, *rest):
    arrays = rest[: 2 * SHIFTS]
    out, a_high, a_low, b_high, b_low, inv_rows, far, changed, y_high, y_low, sems, row_sems = rest[2 * SHIFTS :]
    core = starts[STARTS - 1]
    rows = Rows(starts, row_tiles, slot_count)
    tile = changed.shape[-1]
    first = jnp.where(core == 0, rows.group(0), rows.middle)
    count = jnp.where(core == 0, rows.middle, rows.group(1)) - first
    pairs = [(a_high_in, a_high), (a_low_in, a_low), (b_high_in, b_high), (b_low_in, b_low), (inv_in, inv_rows)]
    base = 0
    bases = []
    for array in arrays:
        bases.append(base)
        pairs.append((array, far.at[pl.ds(base, array.shape[0])]))
        base += array.shape[0]
    copies = [pltpu.make_async_copy(*pair, sems.at[i]) for i, pair in enumerate(pairs)]
    for copy in reversed(copies):
        copy.start()
    targets = []
    for side in range(2):
        sign = -1 if side == 0 else 1
        for i in range(BAND):
            for e in range(1, BAND + 1 - i):
                j = i if side == 0 else count - 1 - i
                t = rows.tile_at(first + j, sign * (i + e))
                targets.append((side, i, e, (i < count) & (t > 0), j * row_tiles + t))
    for at, (side, i, e, present, place) in enumerate(targets):

        @pl.when(present)
        def read():
            pltpu.make_async_copy(estimate.at[place], changed.at[at], row_sems.at[at]).start()

    y_high[...] = jnp.zeros_like(y_high)
    y_low[...] = jnp.zeros_like(y_low)
    for copy in copies[4:]:
        copy.wait()
    for side in range(2):
        direct = core == side
        between = jnp.where(direct, 0, first - rows.group(0) if side == 0 else rows.group(1) - first - count)
        one = rows.group(0) - rows.group(-1) if side == 0 else rows.group(2) - rows.group(1)
        two = rows.group(0) - rows.group(-2) if side == 0 else rows.group(3) - rows.group(1)
        for d, step in FAR:
            e = d - step
            here = (side, pl.ds((d - BAND - 1) * tile, tile), pl.ds((e - 1) * tile, tile))
            beyond = d - between
            place = jnp.int32(0)
            for distance, other_step in FAR:
                if other_step == step and distance <= d:
                    for shift in reversed(range(1, SHIFTS + 1)):
                        slots = far_slots(shift)
                        if (distance, step) in slots:
                            at = slots.index((distance, step))
                            at = jnp.where(direct, bases[shift - 1] + at, bases[SHIFTS + shift - 1] + at)
                            held = jnp.bool_(True) if shift == SHIFTS else beyond <= (one, two)[shift - 1]
                            place = jnp.where((beyond == distance) & held, at, place)
            value = jnp.where(beyond > BAND, far[place] * inv_rows[side * BAND + e - 1], 0.0)
            high_part, low_part = split(value)
            y_high[here] = high_part
            y_low[here] = low_part
    for copy in copies[:4]:
        copy.wait()
    extras = []
    for side in range(2):
        extra = dot(a_high[side], y_high[side]) + dot(a_high[side], y_low[side])
        extras.append(extra + dot(a_low[side], y_high[side]))
    changes = []
    for side in range(2):
        sign = -1 if side == 0 else 1
        bands = []
        for k in range(1, BAND + 1):
            parts = []
            for e in range(1, BAND + 1):
                part = extras[side][(k - 1) * tile : k * tile, (e - 1) * tile : e * tile]
                if k != e:
                    row = first - k if side == 0 else first + count + k - 1
                    part = jnp.where(rows.tile_at(row, sign * (e - k)) > 0, part, 0.0)
                parts.append(part)
            bands.append(jnp.concatenate(parts, axis=1))
        extra_high, extra_low = split(jnp.concatenate(bands, axis=0))
        change = dot(b_high[side], extra_high) + dot(b_high[side], extra_low)
        changes.append(change + dot(b_low[side], extra_high))
    for at, (side, i, e, present, place) in enumerate(targets):
        part = changes[side][i * tile : (i + 1) * tile, (e - 1) * tile : e * tile]

        @pl.when(present)
        def update():
            pltpu.make_async_copy(estimate.at[place], changed.at[at], row_sems.at[at]).wait()
            changed[at] -= part
            pltpu.make_async_copy(changed.at[at], out.at[place], row_sems.at[at]).start()

    for at, (side, i, e, present, place) in enumerate(targets):

        @pl.when(present)
        def finish():
            pltpu.make_async_copy(changed.at[at], out.at[place], row_sems.at[at]).wait()


def estimate_rows(coupling, columns, row_slots):
    slot_count, row_tiles, tile, _ = coupling.shape
    devices = lax.axis_size("rows")
    own_index = lax.axis_index("rows")
    held = slot_count * row_tiles
    near = slot_count + 2 * BAND
    width = 2 * BAND + 1
    reach = BAND * tile
    own = coupling.reshape(held, tile, tile)
    listed = range(devices)
    smem = pl.BlockSpec(memory_space=pltpu.SMEM)
    hbm = pl.BlockSpec(memory_space=pl.ANY)
    vmem = pl.BlockSpec(memory_space=pltpu.VMEM)

    def blocks(count, dtype=jnp.float32):
        return jax.ShapeDtypeStruct((count, tile, tile), dtype)

    def partner(value):
        return lax.ppermute(value, "rows", [(i, i ^ 1) for i in listed])

    def along(value, step):
        return lax.ppermute(value, "rows", [(i, (i + (-step if i % GROUP else step)) % devices) for i in listed])

    other = partner(own)
    mine = (row_slots >= own_index * slot_count) & (row_slots < (own_index + 1) * slot_count)
    last = jnp.sum(mine.astype(jnp.int32)) - 1
    edge_row = jnp.where(own_index % GROUP == 0, 0, last) * row_tiles
    edge_out = lax.dynamic_slice_in_dim(own, edge_row, row_tiles, 0)
    edge = along(edge_out, -1)
    starts = group_starts(lax.optimization_barrier((row_slots, edge_out))[0], slot_count, devices, own_index)
    near_out, next_out = pl.pallas_call(
        lambda *refs: near_pack_kernel(row_tiles, slot_count, *refs),
        out_shape=[blocks((BAND - 1) * row_tiles), blocks(row_tiles)],
        in_specs=[smem] + [hbm] * 2,
        out_specs=[vmem] * 2,
        scratch_shapes=[pltpu.SemaphoreType.DMA((BAND,))],
        compiler_params=pltpu.CompilerParams(vmem_limit_bytes=4 * 2**20),
        name="near_pack",
    )(starts, own, other)
    near_rows = along(near_out, GROUP)
    next_rows = along(next_out, 2 * GROUP)
    table = pattern_table(lax.optimization_barrier((starts, near_out))[0], row_slots, columns, slot_count)
    far_out = pl.pallas_call(
        lambda *refs: far_pack_kernel(row_tiles, slot_count, *refs),
        out_shape=[blocks(len(far_slots(shift))) for shift in range(1, SHIFTS + 1)],
        in_specs=[smem] + [hbm] * 2,
        out_specs=[vmem] * SHIFTS,
        scratch_shapes=[
            pltpu.VMEM((GROUP * held, tile, tile), jnp.float32),
            pltpu.SemaphoreType.DMA((2,)),
        ],
        compiler_params=pltpu.CompilerParams(vmem_limit_bytes=8 * 2**20),
        name="far_pack",
    )(table, own, other)
    passed = []
    for value in (edge, near_rows, next_rows):
        passed.append(partner(value))
    far_out = lax.optimization_barrier((tuple(far_out), near_rows))[0]
    far_in = []
    for shift in range(1, SHIFTS + 1):
        far_in.append(along(far_out[shift - 1], GROUP * shift))
    rows_of = near * row_tiles
    table_size = (near + 2 * BAND) * width
    side_block = jax.ShapeDtypeStruct((2, reach, reach), jnp.bfloat16)
    estimate, *shares = pl.pallas_call(
        lambda *refs: near_kernel(row_tiles, slot_count, *refs),
        out_shape=[blocks(held)] + [side_block] * 4 + [jax.ShapeDtypeStruct((2 * BAND, 1, tile), jnp.float32)],
        in_specs=[smem] + [hbm] * 8,
        out_specs=[vmem] * 6,
        scratch_shapes=[
            pltpu.VMEM(((near + 2 * BAND) * row_tiles, tile, tile), jnp.float32),
            pltpu.VMEM((near, tile, row_tiles * tile), jnp.bfloat16),
            pltpu.VMEM((near, tile, row_tiles * tile), jnp.bfloat16),
            pltpu.VMEM((table_size + 1, tile, tile), jnp.bfloat16),
            pltpu.VMEM((table_size + 1, tile, tile), jnp.bfloat16),
            pltpu.VMEM((rows_of + 1, tile, tile), jnp.bfloat16),
            pltpu.VMEM((rows_of + 1, tile, tile), jnp.bfloat16),
            pltpu.VMEM((near, 1, tile), jnp.float32),
            pltpu.SMEM((rows_of,), jnp.int32),
            pltpu.SMEM((table_size,), jnp.int32),
            pltpu.SMEM((near * width,), jnp.int32),
            pltpu.SMEM((near + 2 * BAND,), jnp.int32),
            pltpu.SemaphoreType.DMA((near + 2 * BAND,)),
        ],
        cost_estimate=pl.CostEstimate(flops=4 * 10**9, bytes_accessed=10**7, transcendentals=0),
        compiler_params=pltpu.CompilerParams(vmem_limit_bytes=30 * 2**20),
        name="near_rows",
    )(table, own, other, edge, near_rows, next_rows, *passed)
    far_passed = []
    for shift in range(1, SHIFTS + 1):
        far_passed.append(partner(far_in[shift - 1]))
    targets = BAND * (BAND + 1)
    out = pl.pallas_call(
        lambda *refs: far_kernel(row_tiles, slot_count, *refs),
        out_shape=blocks(held),
        in_specs=[smem] + [hbm] * (6 + 2 * SHIFTS),
        out_specs=hbm,
        scratch_shapes=[pltpu.VMEM((2, reach, reach), jnp.bfloat16)] * 4
        + [
            pltpu.VMEM((2 * BAND, 1, tile), jnp.float32),
            pltpu.VMEM((2 * sum(len(far_slots(shift)) for shift in range(1, SHIFTS + 1)), tile, tile), jnp.float32),
            pltpu.VMEM((targets, tile, tile), jnp.float32),
            pltpu.VMEM((2, reach, reach), jnp.bfloat16),
            pltpu.VMEM((2, reach, reach), jnp.bfloat16),
            pltpu.SemaphoreType.DMA((5 + 2 * SHIFTS,)),
            pltpu.SemaphoreType.DMA((targets,)),
        ],
        input_output_aliases={1: 0},
        compiler_params=pltpu.CompilerParams(vmem_limit_bytes=12 * 2**20),
        name="far_rows",
    )(table, estimate, *shares, *far_in, *far_passed)
    return out.reshape(coupling.shape)


def solution(mesh):
    return jax.shard_map(
        estimate_rows,
        mesh=mesh,
        in_specs=(P("rows", None, None, None), P(), P()),
        out_specs=P("rows", None, None, None),
        check_vma=False,
    )
```

```python
import jax
import jax.numpy as jnp
from jax import lax
from jax.experimental import pallas as pl
from jax.experimental.pallas import tpu as pltpu
from jax.sharding import PartitionSpec as P


BAND = 3
REACH = 2 * BAND
GROUP = 2
SHIFTS = 3
STARTS = 2 * SHIFTS + 4

FAR = [(d, step) for d in range(BAND + 1, REACH + 1) for step in range(d - BAND, BAND + 1)]


def far_slots(shift):
    return [(d, step) for d, step in FAR if d > GROUP * (shift - 1)]


def group_starts(row_slots, slot_count, devices, own_index):
    groups = devices // GROUP
    group = own_index // GROUP
    steps = jnp.arange(-SHIFTS, SHIFTS + 2, dtype=jnp.int32)
    wanted = group + steps
    turns = jnp.floor_divide(wanted, groups)
    firsts = jnp.concatenate([(wanted - turns * groups) * GROUP, group[None] * GROUP + 1])
    turns = jnp.concatenate([turns, jnp.zeros((1,), jnp.int32)])
    below = (row_slots[None, :] < (firsts * slot_count)[:, None]).astype(jnp.int32)
    starts = jnp.sum(below, axis=1) + turns * row_slots.shape[0]
    return jnp.concatenate([starts, (own_index % GROUP)[None]])


def pattern_table(starts, row_slots, columns, slot_count):
    rows = row_slots.shape[0]
    span = GROUP * slot_count + 2 * REACH
    row = starts[SHIFTS] - REACH + jnp.arange(span, dtype=jnp.int32)
    row = jnp.where(row < 0, row + rows, row)
    row = jnp.where(row >= rows, row - rows, row)
    found = jnp.take(columns, jnp.take(row_slots, row), axis=0) - row[:, None]
    found = jnp.where(found > rows // 2, found - rows, found)
    found = jnp.where(found < -(rows // 2), found + rows, found)
    wanted = jnp.arange(-BAND, BAND + 1, dtype=jnp.int32)
    order = jnp.arange(1, columns.shape[1] + 1, dtype=jnp.int32)
    which = jnp.sum(jnp.where(found[:, None, :] == wanted[None, :, None], order, 0), axis=2) - 1
    return jnp.concatenate([starts, jnp.clip(found, -BAND, BAND).reshape(-1), which.reshape(-1)])


class Rows:
    def __init__(self, table, row_tiles, slot_count):
        self.table = table
        self.row_tiles = row_tiles
        self.slot_count = slot_count
        self.core = table[STARTS - 1]
        self.middle = table[STARTS - 2]
        self.offsets = STARTS
        self.which = STARTS + (GROUP * slot_count + 2 * REACH) * row_tiles

    def group(self, step):
        return self.table[SHIFTS + step]

    def edge(self, shift, forward):
        return jnp.where(forward, self.group(shift), self.group(1 - shift))

    def place(self, row):
        return jnp.clip(row - self.group(0) + REACH, 0, GROUP * self.slot_count + 2 * REACH - 1)

    def offset(self, row, t):
        return self.table[self.offsets + self.place(row) * self.row_tiles + t]

    def tile_at(self, row, offset):
        return self.table[self.which + self.place(row) * (2 * BAND + 1) + offset + BAND]

    def group_tile(self, row):
        low = self.group(0)
        middle = self.middle
        slot = jnp.where(row < middle, row - low, row - middle + self.slot_count)
        return jnp.clip(slot, 0, GROUP * self.slot_count - 1) * self.row_tiles


def split(value):
    high = value.astype(jnp.bfloat16)
    return high, (value - high.astype(jnp.float32)).astype(jnp.bfloat16)


def eye(tile):
    return lax.broadcasted_iota(jnp.int32, (tile, tile), 0) == lax.broadcasted_iota(
        jnp.int32, (tile, tile), 1
    )


def inverse_column(block):
    tile = block.shape[-1]
    return 1.0 / jnp.sum(jnp.where(eye(tile), block, 0.0), axis=1, keepdims=True)


def inverse_row(block):
    tile = block.shape[-1]
    return 1.0 / jnp.sum(jnp.where(eye(tile), block, 0.0), axis=0, keepdims=True)


def near_pack_kernel(row_tiles, slot_count, starts, own, other, near, next_near, sems):
    rows = Rows(starts, row_tiles, slot_count)
    forward = rows.core == 0
    held = slot_count * row_tiles
    wanted = []
    for shift, ref, distances in ((1, near, range(1, BAND + 1)), (2, next_near, (BAND,))):
        for i, d in enumerate(distances):
            edge = rows.edge(shift, forward)
            base = rows.group_tile(jnp.where(forward, edge - d, edge + d - 1))
            wanted.append((base, ref.at[pl.ds(i * row_tiles, row_tiles)]))
    for i, (base, place) in enumerate(wanted):
        second = base >= held
        mine = jnp.where(second, 1, 0) == rows.core
        start = jnp.where(second, base - held, base)

        @pl.when(mine)
        def take_own():
            pltpu.make_async_copy(own.at[pl.ds(start, row_tiles)], place, sems.at[i]).start()

        @pl.when(jnp.logical_not(mine))
        def take_other():
            pltpu.make_async_copy(other.at[pl.ds(start, row_tiles)], place, sems.at[i]).start()

    for i, (base, place) in enumerate(wanted):
        pltpu.make_async_copy(own.at[pl.ds(0, row_tiles)], place, sems.at[i]).wait()


def far_pack_kernel(row_tiles, slot_count, starts, own, other, *rest):
    outs = rest[:SHIFTS]
    pool, sems = rest[SHIFTS:]
    core = starts[STARTS - 1]
    rows = Rows(starts, row_tiles, slot_count)
    held = slot_count * row_tiles
    own_copy = pltpu.make_async_copy(own, pool.at[pl.ds(core * held, held)], sems.at[0])
    other_copy = pltpu.make_async_copy(other, pool.at[pl.ds((1 - core) * held, held)], sems.at[1])
    own_copy.start()
    other_copy.start()
    own_copy.wait()
    other_copy.wait()
    forward = core == 0
    sign = jnp.where(forward, 1, -1)
    for shift in range(1, SHIFTS + 1):
        edge = rows.edge(shift, forward)
        slots = far_slots(shift)
        for d in sorted({d for d, _ in slots}):
            row = jnp.where(forward, edge - d, edge + d - 1)
            base = rows.group_tile(row)
            scale = -inverse_column(pool[base])
            for at, (distance, step) in enumerate(slots):
                if distance == d:
                    t = rows.tile_at(row, sign * step)
                    factor = jnp.where(t > 0, scale, 0.0)
                    outs[shift - 1][at] = factor * pool[base + jnp.maximum(t, 0)]


def dot(a, b):
    return jnp.dot(a, b, preferred_element_type=jnp.float32)


def near_kernel(row_tiles, slot_count, starts, own, other, near_rows, next_rows,
                near_p, next_p, out, a_high, a_low, b_high, b_low, inv_out,
                pool, left_high, left_low, y_high, y_low, p_high, p_low,
                inv_row, offsets, y_at, p_at, whole, sems):
    core = starts[2 * SHIFTS + 3]
    rows = Rows(starts, row_tiles, slot_count)
    tile = own.shape[-1]
    width = 2 * BAND + 1
    first = jnp.where(core == 0, rows.group(0), rows.middle)
    count = jnp.where(core == 0, rows.middle, rows.group(1)) - first
    near = count + 2 * BAND
    low = rows.group(0)
    high = rows.group(1)
    near_behind = low - rows.group(-1)
    near_ahead = rows.group(2) - high
    zero_y = y_high.shape[0] - 1
    zero_p = p_high.shape[0] - 1
    nothing = jnp.zeros((tile, tile), jnp.bfloat16)
    y_high[zero_y] = nothing
    y_low[zero_y] = nothing
    p_high[zero_p] = nothing
    p_low[zero_p] = nothing

    def fetch(w, carry):
        row = first - REACH + w
        behind = row < low
        ahead = row >= high
        outside = behind | ahead
        inside = jnp.logical_not(outside)
        d = jnp.where(behind, low - row, row - high + 1)
        reached = jnp.where(behind, near_behind, near_ahead)
        mine = outside & (jnp.where(behind, 0, 1) == core)
        theirs = outside & (jnp.where(behind, 0, 1) != core)
        home = inside & (jnp.where(row < rows.middle, 0, 1) == core)
        slot = jnp.where(row < rows.middle, row - low, row - rows.middle)
        whole[w] = jnp.where(inside | (d <= BAND), 1, 0)
        choices = [(home, own, slot), (inside & jnp.logical_not(home), other, slot)]
        for side, refs in ((mine, (near_rows, next_rows)), (theirs, (near_p, next_p))):
            choices.append((side & (d <= BAND) & (d <= reached), refs[0], d - 1))
            choices.append((side & (d == BAND) & (d > reached), refs[1], 0))
        for chosen, ref, at in choices:

            @pl.when(chosen)
            def take():
                pltpu.make_async_copy(
                    ref.at[pl.ds(at * row_tiles, row_tiles)], pool.at[pl.ds(w * row_tiles, row_tiles)], sems.at[w]
                ).start()

        return carry

    lax.fori_loop(0, near + 2 * BAND, fetch, 0)

    def clear_y(i, carry):
        y_at[i] = zero_y
        return carry

    def clear_p(i, carry):
        p_at[i] = zero_p
        return carry

    lax.fori_loop(0, y_at.shape[0], clear_y, 0, unroll=8)
    lax.fori_loop(0, p_at.shape[0], clear_p, 0, unroll=7)

    def arrive(w, carry):
        @pl.when(whole[w] == 1)
        def wait():
            place = pool.at[pl.ds(w * row_tiles, row_tiles)]
            pltpu.make_async_copy(own.at[pl.ds(0, row_tiles)], place, sems.at[w]).wait()

        return carry

    lax.fori_loop(0, near + 2 * BAND, arrive, 0)

    def invert(f, carry):
        inv_row[f] = inverse_row(pool[(f + BAND) * row_tiles])
        return carry

    lax.fori_loop(0, near, invert, 0)

    def near_row(f, carry):
        row = first - BAND + f
        base = (f + BAND) * row_tiles
        column = inverse_column(pool[base])
        for t in range(row_tiles):
            offset = rows.offset(row, t)
            offsets[f * row_tiles + t] = offset
            block = pool[base + t]
            high_part, low_part = split(block)
            left_high[f, :, pl.ds(t * tile, tile)] = high_part
            left_low[f, :, pl.ds(t * tile, tile)] = low_part
            c = f + offset
            inside = (c >= 0) & (c < near)
            value = -(column * block) * inv_row[jnp.clip(c, 0, near - 1)]
            if t == 0:
                value = value + jnp.where(eye(tile), 2.0 * column, 0.0)
            high_part, low_part = split(value)
            at = (f + BAND) * width + offset + BAND
            y_high[at] = high_part
            y_low[at] = low_part
            y_at[at] = jnp.where(inside, at, zero_y)
            p_at[f * width + offset + BAND] = f * row_tiles + t
        return carry

    lax.fori_loop(0, near, near_row, 0)

    def far_row(e, carry):
        behind = e < BAND
        sign = jnp.where(behind, 1, -1)
        d = jnp.where(behind, REACH - e, e + 1)
        w = jnp.where(behind, e, near + e)
        row = first - REACH + w

        @pl.when(whole[w] == 1)
        def build():
            scale = -inverse_column(pool[w * row_tiles])
            for step in range(1, BAND + 1):
                offset = sign * step
                t = rows.tile_at(row, offset)
                at = w * width + offset + BAND

                @pl.when((t > 0) & (step >= d - BAND))
                def keep():
                    c = jnp.clip(w - BAND + offset, 0, near - 1)
                    high_part, low_part = split((scale * pool[w * row_tiles + t]) * inv_row[c])
                    y_high[at] = high_part
                    y_low[at] = low_part
                    y_at[at] = at

        return carry

    lax.fori_loop(0, 2 * BAND, far_row, 0)

    def gathered(table, start, zero, high_ref, low_ref, f, lefts):
        steps = [offsets[f * row_tiles + t] for t in range(row_tiles)]
        at = []
        for t in range(row_tiles):
            line = []
            for v in range(row_tiles):
                ahead = steps[v] - steps[t]
                inside = (ahead >= -BAND) & (ahead <= BAND)
                place = (start + steps[t]) * width + jnp.clip(ahead, -BAND, BAND) + BAND
                line.append(jnp.where(inside, table[place], zero))
            at.append(line)
        left_h, left_l = lefts
        results = []
        for v in range(0, row_tiles, 2):
            pair = range(v, min(v + 2, row_tiles))

            def right(ref):
                lines = [jnp.concatenate([ref[at[t][c]] for c in pair], axis=1) for t in range(row_tiles)]
                return jnp.concatenate(lines, axis=0)

            high_right = right(high_ref)
            rights = jnp.concatenate([high_right, high_right, right(low_ref)], axis=0)
            value = dot(jnp.concatenate([left_h, left_l, left_h], axis=1), rights)
            for i in range(len(pair)):
                results.append(value[:, i * tile : (i + 1) * tile])
        return results

    def product_row(f, carry):
        values = gathered(y_at, f + BAND, zero_y, y_high, y_low, f, (left_high[f], left_low[f]))
        for t, value in enumerate(values):
            high_part, low_part = split(value)
            p_high[f * row_tiles + t] = high_part
            p_low[f * row_tiles + t] = low_part
        return carry

    lax.fori_loop(0, near, product_row, 0)

    def own_row(j, carry):
        f = j + BAND
        tiles = []
        for t in range(row_tiles):
            at = (f + BAND) * width + offsets[f * row_tiles + t] + BAND
            tiles.append((y_high[at], y_low[at]))
        lefts = [jnp.concatenate([pair[i] for pair in tiles], axis=1) for i in range(2)]
        values = gathered(p_at, f, zero_p, p_high, p_low, f, lefts)
        for t, value in enumerate(values):
            high_part, low_part = tiles[t]
            out[j * row_tiles + t] = 2.0 * (high_part.astype(jnp.float32) + low_part.astype(jnp.float32)) - value
        return carry

    lax.fori_loop(0, count, own_row, 0)

    def empty_row(j, carry):
        for t in range(row_tiles):
            out[j * row_tiles + t] = jnp.zeros((tile, tile), jnp.float32)
        return carry

    lax.fori_loop(count, slot_count, empty_row, 0)

    a_high[...] = jnp.zeros_like(a_high)
    a_low[...] = jnp.zeros_like(a_low)
    b_high[...] = jnp.zeros_like(b_high)
    b_low[...] = jnp.zeros_like(b_low)
    for side in range(2):
        sign = -1 if side == 0 else 1
        for e in range(1, BAND + 1):
            f = BAND - e if side == 0 else near - BAND + e - 1
            row = first - BAND + f
            inv_out[side * BAND + e - 1] = inv_row[f]
            for d in range(BAND + 1, REACH + 1):
                if d - e <= BAND:
                    t = rows.tile_at(row, sign * (d - e))
                    here = (side, pl.ds((e - 1) * tile, tile), pl.ds((d - BAND - 1) * tile, tile))

                    @pl.when(t > 0)
                    def keep_a():
                        lanes = pl.ds(pl.multiple_of(t * tile, tile), tile)
                        a_high[here] = left_high[f, :, lanes]
                        a_low[here] = left_low[f, :, lanes]

            for i in range(BAND + 1 - e):
                w = REACH + i if side == 0 else REACH + count - 1 - i
                at = y_at[w * width + sign * (i + e) + BAND]
                here = (side, pl.ds(i * tile, tile), pl.ds((e - 1) * tile, tile))

                @pl.when(i < count)
                def keep_b():
                    b_high[here] = y_high[at]
                    b_low[here] = y_low[at]


def far_kernel(row_tiles, slot_count, starts, estimate, a_high_in, a_low_in, b_high_in, b_low_in, inv_in, *rest):
    arrays = rest[: 2 * SHIFTS]
    out, a_high, a_low, b_high, b_low, inv_rows, far, changed, y_high, y_low, sems, row_sems = rest[2 * SHIFTS :]
    core = starts[STARTS - 1]
    rows = Rows(starts, row_tiles, slot_count)
    tile = changed.shape[-1]
    first = jnp.where(core == 0, rows.group(0), rows.middle)
    count = jnp.where(core == 0, rows.middle, rows.group(1)) - first
    pairs = [(a_high_in, a_high), (a_low_in, a_low), (b_high_in, b_high), (b_low_in, b_low), (inv_in, inv_rows)]
    base = 0
    bases = []
    for array in arrays:
        bases.append(base)
        pairs.append((array, far.at[pl.ds(base, array.shape[0])]))
        base += array.shape[0]
    copies = [pltpu.make_async_copy(*pair, sems.at[i]) for i, pair in enumerate(pairs)]
    for copy in reversed(copies):
        copy.start()
    targets = []
    for side in range(2):
        sign = -1 if side == 0 else 1
        for i in range(BAND):
            for e in range(1, BAND + 1 - i):
                j = i if side == 0 else count - 1 - i
                t = rows.tile_at(first + j, sign * (i + e))
                targets.append((side, i, e, (i < count) & (t > 0), j * row_tiles + t))
    for at, (side, i, e, present, place) in enumerate(targets):

        @pl.when(present)
        def read():
            pltpu.make_async_copy(estimate.at[place], changed.at[at], row_sems.at[at]).start()

    y_high[...] = jnp.zeros_like(y_high)
    y_low[...] = jnp.zeros_like(y_low)
    for copy in copies[4:]:
        copy.wait()
    for side in range(2):
        direct = core == side
        between = jnp.where(direct, 0, first - rows.group(0) if side == 0 else rows.group(1) - first - count)
        one = rows.group(0) - rows.group(-1) if side == 0 else rows.group(2) - rows.group(1)
        two = rows.group(0) - rows.group(-2) if side == 0 else rows.group(3) - rows.group(1)
        for d, step in FAR:
            e = d - step
            here = (side, pl.ds((d - BAND - 1) * tile, tile), pl.ds((e - 1) * tile, tile))
            beyond = d - between
            place = jnp.int32(0)
            for distance, other_step in FAR:
                if other_step == step and distance <= d:
                    for shift in reversed(range(1, SHIFTS + 1)):
                        slots = far_slots(shift)
                        if (distance, step) in slots:
                            at = slots.index((distance, step))
                            at = jnp.where(direct, bases[shift - 1] + at, bases[SHIFTS + shift - 1] + at)
                            held = jnp.bool_(True) if shift == SHIFTS else beyond <= (one, two)[shift - 1]
                            place = jnp.where((beyond == distance) & held, at, place)
            value = jnp.where(beyond > BAND, far[place] * inv_rows[side * BAND + e - 1], 0.0)
            high_part, low_part = split(value)
            y_high[here] = high_part
            y_low[here] = low_part
    for copy in copies[:4]:
        copy.wait()
    extras = []
    for side in range(2):
        extra = dot(a_high[side], y_high[side]) + dot(a_high[side], y_low[side])
        extras.append(extra + dot(a_low[side], y_high[side]))
    changes = []
    for side in range(2):
        sign = -1 if side == 0 else 1
        bands = []
        for k in range(1, BAND + 1):
            parts = []
            for e in range(1, BAND + 1):
                part = extras[side][(k - 1) * tile : k * tile, (e - 1) * tile : e * tile]
                if k != e:
                    row = first - k if side == 0 else first + count + k - 1
                    part = jnp.where(rows.tile_at(row, sign * (e - k)) > 0, part, 0.0)
                parts.append(part)
            bands.append(jnp.concatenate(parts, axis=1))
        extra_high, extra_low = split(jnp.concatenate(bands, axis=0))
        change = dot(b_high[side], extra_high) + dot(b_high[side], extra_low)
        changes.append(change + dot(b_low[side], extra_high))
    for at, (side, i, e, present, place) in enumerate(targets):
        part = changes[side][i * tile : (i + 1) * tile, (e - 1) * tile : e * tile]

        @pl.when(present)
        def update():
            pltpu.make_async_copy(estimate.at[place], changed.at[at], row_sems.at[at]).wait()
            changed[at] -= part
            pltpu.make_async_copy(changed.at[at], out.at[place], row_sems.at[at]).start()

    for at, (side, i, e, present, place) in enumerate(targets):

        @pl.when(present)
        def finish():
            pltpu.make_async_copy(changed.at[at], out.at[place], row_sems.at[at]).wait()


def estimate_rows(coupling, columns, row_slots):
    slot_count, row_tiles, tile, _ = coupling.shape
    devices = lax.axis_size("rows")
    own_index = lax.axis_index("rows")
    held = slot_count * row_tiles
    near = slot_count + 2 * BAND
    width = 2 * BAND + 1
    reach = BAND * tile
    own = coupling.reshape(held, tile, tile)
    listed = range(devices)
    smem = pl.BlockSpec(memory_space=pltpu.SMEM)
    hbm = pl.BlockSpec(memory_space=pl.ANY)
    vmem = pl.BlockSpec(memory_space=pltpu.VMEM)

    def blocks(count, dtype=jnp.float32):
        return jax.ShapeDtypeStruct((count, tile, tile), dtype)

    def partner(value):
        return lax.ppermute(value, "rows", [(i, i ^ 1) for i in listed])

    def along(value, step):
        return lax.ppermute(value, "rows", [(i, (i + (-step if i % GROUP else step)) % devices) for i in listed])

    other = partner(own)
    starts = group_starts(row_slots, slot_count, devices, own_index)
    near_out, next_out = pl.pallas_call(
        lambda *refs: near_pack_kernel(row_tiles, slot_count, *refs),
        out_shape=[blocks(BAND * row_tiles), blocks(row_tiles)],
        in_specs=[smem] + [hbm] * 2,
        out_specs=[vmem] * 2,
        scratch_shapes=[pltpu.SemaphoreType.DMA((BAND + 1,))],
        compiler_params=pltpu.CompilerParams(vmem_limit_bytes=4 * 2**20),
        name="near_pack",
    )(starts, own, other)
    near_rows = along(near_out, GROUP)
    next_rows = along(next_out, 2 * GROUP)
    table = pattern_table(lax.optimization_barrier((starts, near_out))[0], row_slots, columns, slot_count)
    far_out = pl.pallas_call(
        lambda *refs: far_pack_kernel(row_tiles, slot_count, *refs),
        out_shape=[blocks(len(far_slots(shift))) for shift in range(1, SHIFTS + 1)],
        in_specs=[smem] + [hbm] * 2,
        out_specs=[vmem] * SHIFTS,
        scratch_shapes=[
            pltpu.VMEM((GROUP * held, tile, tile), jnp.float32),
            pltpu.SemaphoreType.DMA((2,)),
        ],
        compiler_params=pltpu.CompilerParams(vmem_limit_bytes=8 * 2**20),
        name="far_pack",
    )(table, own, other)
    passed = []
    for value in (near_rows, next_rows):
        passed.append(partner(value))
    far_out = lax.optimization_barrier((tuple(far_out), near_rows))[0]
    far_in = []
    for shift in range(1, SHIFTS + 1):
        far_in.append(along(far_out[shift - 1], GROUP * shift))
    rows_of = near * row_tiles
    table_size = (near + 2 * BAND) * width
    side_block = jax.ShapeDtypeStruct((2, reach, reach), jnp.bfloat16)
    estimate, *shares = pl.pallas_call(
        lambda *refs: near_kernel(row_tiles, slot_count, *refs),
        out_shape=[blocks(held)] + [side_block] * 4 + [jax.ShapeDtypeStruct((2 * BAND, 1, tile), jnp.float32)],
        in_specs=[smem] + [hbm] * 6,
        out_specs=[vmem] * 6,
        scratch_shapes=[
            pltpu.VMEM(((near + 2 * BAND) * row_tiles, tile, tile), jnp.float32),
            pltpu.VMEM((near, tile, row_tiles * tile), jnp.bfloat16),
            pltpu.VMEM((near, tile, row_tiles * tile), jnp.bfloat16),
            pltpu.VMEM((table_size + 1, tile, tile), jnp.bfloat16),
            pltpu.VMEM((table_size + 1, tile, tile), jnp.bfloat16),
            pltpu.VMEM((rows_of + 1, tile, tile), jnp.bfloat16),
            pltpu.VMEM((rows_of + 1, tile, tile), jnp.bfloat16),
            pltpu.VMEM((near, 1, tile), jnp.float32),
            pltpu.SMEM((rows_of,), jnp.int32),
            pltpu.SMEM((table_size,), jnp.int32),
            pltpu.SMEM((near * width,), jnp.int32),
            pltpu.SMEM((near + 2 * BAND,), jnp.int32),
            pltpu.SemaphoreType.DMA((near + 2 * BAND,)),
        ],
        cost_estimate=pl.CostEstimate(flops=4 * 10**9, bytes_accessed=10**7, transcendentals=0),
        compiler_params=pltpu.CompilerParams(vmem_limit_bytes=30 * 2**20),
        name="near_rows",
    )(table, own, other, near_rows, next_rows, *passed)
    far_passed = []
    for shift in range(1, SHIFTS + 1):
        far_passed.append(partner(far_in[shift - 1]))
    targets = BAND * (BAND + 1)
    out = pl.pallas_call(
        lambda *refs: far_kernel(row_tiles, slot_count, *refs),
        out_shape=blocks(held),
        in_specs=[smem] + [hbm] * (6 + 2 * SHIFTS),
        out_specs=hbm,
        scratch_shapes=[pltpu.VMEM((2, reach, reach), jnp.bfloat16)] * 4
        + [
            pltpu.VMEM((2 * BAND, 1, tile), jnp.float32),
            pltpu.VMEM((2 * sum(len(far_slots(shift)) for shift in range(1, SHIFTS + 1)), tile, tile), jnp.float32),
            pltpu.VMEM((targets, tile, tile), jnp.float32),
            pltpu.VMEM((2, reach, reach), jnp.bfloat16),
            pltpu.VMEM((2, reach, reach), jnp.bfloat16),
            pltpu.SemaphoreType.DMA((5 + 2 * SHIFTS,)),
            pltpu.SemaphoreType.DMA((targets,)),
        ],
        input_output_aliases={1: 0},
        compiler_params=pltpu.CompilerParams(vmem_limit_bytes=12 * 2**20),
        name="far_rows",
    )(table, estimate, *shares, *far_in, *far_passed)
    return out.reshape(coupling.shape)


def solution(mesh):
    return jax.shard_map(
        estimate_rows,
        mesh=mesh,
        in_specs=(P("rows", None, None, None), P(), P()),
        out_specs=P("rows", None, None, None),
        check_vma=False,
    )
```
